32 devices in a mesh: rep: 2 (over z, core), dp: 16 (over x, y).
Axes of the slice: x: 4, y: 4, z: 1, core: 2. Of those that a mesh axis runs over, the one named last changes fastest.
The devices are a block of a 4x4x8 slice.
Arguments:
- x: bfloat16 [32, 4096, 512], P(('rep', 'dp')), parts along dimension 0
- dy: bfloat16 [32, 4096, 512], P(('rep', 'dp')), parts along dimension 0
- w_gate: bfloat16 [2, 512, 1408], P(None, 'dp')
- w_up: bfloat16 [2, 512, 1408], P(None, 'dp')
- w_down: bfloat16 [2, 1408, 512], P(None, 'dp')
- m_w_gate: float32 [2, 512, 1408], P(None, 'dp')
- m_w_up: float32 [2, 512, 1408], P(None, 'dp')
- m_w_down: float32 [2, 1408, 512], P(None, 'dp')
- v_w_gate: float32 [2, 512, 1408], P(None, 'dp')
- v_w_up: float32 [2, 512, 1408], P(None, 'dp')
- v_w_down: float32 [2, 1408, 512], P(None, 'dp')
Outputs:
- output 1: bfloat16 [4, 512, 1408], P('rep', 'dp'), parts along dimension 0
- output 2: bfloat16 [4, 512, 1408], P('rep', 'dp'), parts along dimension 0
- output 3: bfloat16 [4, 1408, 512], P('rep', 'dp'), parts along dimension 0
- output 4: float32 [4, 512, 1408], P('rep', 'dp'), parts along dimension 0
- output 5: float32 [4, 512, 1408], P('rep', 'dp'), parts along dimension 0
- output 6: float32 [4, 1408, 512], P('rep', 'dp'), parts along dimension 0
- output 7: float32 [4, 512, 1408], P('rep', 'dp'), parts along dimension 0
- output 8: float32 [4, 512, 1408], P('rep', 'dp'), parts along dimension 0
- output 9: float32 [4, 1408, 512], P('rep', 'dp'), parts along dimension 0
There are 2 independent parts. The reference program is written for one: setup_inputs(seed, part) draws one part's arguments, and reference() takes and returns one part's arrays. A program takes and returns all parts, laid end to end along the dimension named above; an argument that names none is the same for every part.
All inputs are finite; a program needn't handle non-finite values.
Results may differ from the reference program's by a relative error of at most 0.022.
Values are sent between devices in bfloat16 or wider.
A program may use at most 768 MiB of HBM per device.

```python
import jax
import jax.numpy as jnp
from jax import lax

SEQUENCES = 16
TOKENS = 4096
D = 512
FF = 1408
LAYERS = 2
NAMES = ("w_gate", "w_up", "w_down")
SHAPES = {"w_gate": (LAYERS, D, FF), "w_up": (LAYERS, D, FF), "w_down": (LAYERS, FF, D)}


def bump(key, n, height):
    away = (jnp.arange(n, dtype=jnp.int32) - jax.random.randint(key, (), 0, n, jnp.int32)) % n
    return jnp.where(away < n // 8, height, 1.0)


def together(key, own, strength):
    shared = jax.random.normal(key, own.shape[1:], jnp.float32)
    return (own + strength * shared) * lax.rsqrt(1 + strength * strength)


def setup_inputs(seed: int = 0, part: int = 0) -> dict:
    kx, kdy, ka, kb, kz, kf, kh, kl, *keys = jax.random.split(jax.random.key(seed), 8 + 3 * len(NAMES))
    kx, kdy, ka, kb = (jax.random.fold_in(k, part) for k in (kx, kdy, ka, kb))
    kw, km, kv = (keys[i::3] for i in range(3))
    shape = (SEQUENCES, TOKENS, D)
    much_x, much_dy = jax.random.uniform(kz, (2,), jnp.float32, 0.0, 1.0)
    loud = 2.0 ** jax.random.uniform(jax.random.fold_in(kz, 1), (), jnp.float32, -1.0, 2.0)
    layers = 2.0 ** jax.random.uniform(kl, (LAYERS, 1, 1), jnp.float32, -1.0, 1.0)
    x = together(ka, jax.random.normal(kx, shape, jnp.float32), much_x) * bump(kf, D, 4.0)
    dy = together(kb, jax.random.normal(kdy, shape, jnp.float32), much_dy)
    drawn = {"x": x.astype(jnp.bfloat16), "dy": (loud * dy * (SEQUENCES * TOKENS) ** -0.5).astype(jnp.bfloat16)}
    for key, name in zip(kw, NAMES, strict=True):
        w = jax.random.normal(key, SHAPES[name], jnp.float32) * SHAPES[name][1] ** -0.5
        drawn[name] = (w * {"w_gate": 1.0, "w_up": bump(kh, FF, 4.0), "w_down": layers}[name]).astype(jnp.bfloat16)
    for key, name in zip(km, NAMES, strict=True):
        drawn[f"m_{name}"] = 0.1 * jax.random.normal(key, SHAPES[name], jnp.float32)
    for key, name in zip(kv, NAMES, strict=True):
        drawn[f"v_{name}"] = jax.random.uniform(key, SHAPES[name], jnp.float32, 0.005, 0.015)
    return drawn


def matmul(a, w):
    return jnp.dot(a, w, preferred_element_type=jnp.float32).astype(jnp.bfloat16)


def normed(h):
    wide = h.astype(jnp.float32)
    scale = lax.rsqrt(jnp.mean(wide**2, -1, keepdims=True) + 1e-6)
    return (wide * scale).astype(jnp.bfloat16)


def layer(h, w):
    a = normed(h)
    gate = jnp.dot(a, w["w_gate"], preferred_element_type=jnp.float32)
    up = jnp.dot(a, w["w_up"], preferred_element_type=jnp.float32)
    return h + matmul((jax.nn.silu(gate) * up).astype(jnp.bfloat16), w["w_down"])


def adamw(w, m, v, g):
    m = 0.9 * m + 0.1 * g
    v = 0.95 * v + 0.05 * g * g
    step = m * lax.rsqrt(v + 1e-8) + 0.1 * w
    return (w - 0.02 * step).astype(jnp.bfloat16), m, v


def clipped(gradients, sum_of_squares, count):
    factor = jnp.minimum(1.0, 0.5 * lax.rsqrt(sum_of_squares / count + 1e-30))
    return [g * factor for g in gradients]


def stack(weights, h):
    return lax.scan(lambda h, w: (layer(h, w), None), h, weights)[0]


def reference(x, dy, w_gate, w_up, w_down, m_w_gate, m_w_up, m_w_down, v_w_gate, v_w_up, v_w_down):
    weights = dict(zip(NAMES, (w_gate, w_up, w_down), strict=True))

    def take(so_far, sequence):
        h, by_y = sequence
        _, back = jax.vjp(lambda w: stack(w, h), weights)
        return jax.tree.map(lambda total, term: total + term.astype(jnp.float32), so_far, back(by_y)[0]), None

    none_yet = {name: jnp.zeros(w.shape, jnp.float32) for name, w in weights.items()}
    by_weights, _ = lax.scan(take, none_yet, (x, dy))
    gradients = [by_weights[name].astype(jnp.bfloat16).astype(jnp.float32) for name in NAMES]
    gradients = clipped(gradients, sum(jnp.sum(g * g) for g in gradients), sum(g.size for g in gradients))
    new = [
        adamw(w.astype(jnp.float32), m, v, g)
        for w, m, v, g in zip((w_gate, w_up, w_down), (m_w_gate, m_w_up, m_w_down), (v_w_gate, v_w_up, v_w_down), gradients, strict=True)
    ]
    return tuple(one[which] for which in range(3) for one in new)
```

```python
import functools

import jax
import jax.numpy as jnp
from jax import lax
from jax.experimental import pallas as pl
from jax.experimental.pallas import tpu as pltpu
from jax.sharding import PartitionSpec as P

F32, BF = jnp.float32, jnp.bfloat16
MESH = pl.DeviceIdType.MESH
LANE = 128
TILE = 512
SIDE = 4
STEPS = "ABCD"


def dot(a, b, ca=1, cb=0):
    return lax.dot_general(a, b, (((ca,), (cb,)), ((), ())), preferred_element_type=F32)


def inverse_rms(wide):
    return lax.rsqrt(jnp.mean(wide * wide, -1, keepdims=True) + 1e-6)


def place():
    me = lax.axis_index("dp")
    return me // SIDE, lax.rem(me, SIDE)


def shifted(i, by):
    return lax.rem(i + by + SIDE, SIDE)


def along(order, by, second=False):
    x, y = place()
    if (order == "y") != second:
        return {"dp": x * SIDE + shifted(y, by)}
    return {"dp": shifted(x, by) * SIDE + y}


def ring_places(order):
    x, y = place()
    return (y, x) if order == "y" else (x, y)


def entry_barrier(peers):
    barrier = pltpu.get_barrier_semaphore()
    for peer in peers:
        pl.semaphore_signal(barrier, inc=1, device_id=peer, device_id_type=MESH)
    pl.semaphore_wait(barrier, len(peers))


def neighbours():
    return [along("y", 1), along("y", -1), along("x", 1), along("x", -1)]


class Gather:
    def __init__(self, buf, core, cut, rows, send, recv, base):
        self.buf, self.core, self.send, self.recv, self.base = buf, core, send, recv, base
        half = buf.shape[-1] // 2
        self.half, self.rows, self.r = half, rows, buf.shape[-2]
        self.columns = {"y": (0, cut), "x": (cut, half - cut)}

    def at(self, order, first, second, rows=slice(None)):
        off, width = self.columns[order]
        cols = pl.ds(pl.multiple_of(self.core * self.half + off, LANE), width)
        a, b = (second, first) if order == "y" else (first, second)
        return self.buf.at[a, b, rows, cols]

    def copies(self, step):
        out = []
        for which, order in enumerate("yx"):
            i1, i2 = ring_places(order)
            if step == "A":
                refs = [self.at(order, i1, i2)] * 2
            elif step == "B":
                refs = [
                    self.at(order, shifted(i1, -1), i2, pl.ds(0, self.rows)),
                    self.at(order, shifted(i1, 1), i2, pl.ds(self.rows, self.r - self.rows)),
                ]
            elif step == "C":
                refs = [self.at(order, slice(None), i2)] * 2
            else:
                refs = [
                    self.at(order, pl.ds(0, SIDE // 2), shifted(i2, -1)),
                    self.at(order, pl.ds(SIDE // 2, SIDE // 2), shifted(i2, 1)),
                ]
            for side, ref in enumerate(refs):
                number = self.base + STEPS.index(step) * 4 + which * 2 + side
                out.append(
                    pltpu.make_async_remote_copy(
                        src_ref=ref,
                        dst_ref=ref,
                        send_sem=self.send.at[number],
                        recv_sem=self.recv.at[number],
                        device_id=along(order, 1 - 2 * side, step in "CD"),
                        device_id_type=MESH,
                    )
                )
        return out

    def across(self, partner):
        ref = self.buf.at[:, :, :, pl.ds(pl.multiple_of(self.core * self.half, LANE), self.half)]
        number = self.base + 16
        return pltpu.make_async_remote_copy(
            src_ref=ref, dst_ref=ref, send_sem=self.send.at[number], recv_sem=self.recv.at[number], device_id=partner, device_id_type=MESH
        )

    def advance(self, step, partner):
        if step != "A":
            for copy in self.copies("ABCDE"["ABCDE".index(step) - 1]):
                copy.wait_recv()
        if step == "E":
            self.across(partner).start()
        else:
            for copy in self.copies(step):
                copy.start()

    def finish(self, partner):
        self.across(partner).wait_recv()

    def drain(self, partner):
        for step in STEPS:
            for copy in self.copies(step):
                copy.wait_send()
        self.across(partner).wait_send()


def forward_kernel(layers, wg_ref, wu_ref, wd_ref, x_ref, h_ref, *refs):
    (ogu, od), (gu, dd, wide_d, wd0, send, recv, out_sem) = (refs[:layers], refs[layers : 2 * layers]), refs[2 * layers :]
    step, steps = pl.program_id(0), pl.num_programs(0)
    ff = wg_ref.shape[2]
    rep = lax.axis_index("rep")
    core = lax.rem(rep, 2)
    partner = {"rep": rep + 1 - 2 * core}
    x, y = place()
    units = []
    for layer in range(layers):
        n = 2 * layer
        units.append(Gather(gu.at[layer], core, (gu.shape[-1] // 4 + LANE - 1) // LANE * LANE, 16, send, recv, 17 * n))
        units.append(Gather(dd.at[layer], core, dd.shape[-1] // 4, 48, send, recv, 17 * (n + 1)))
    first, rest = units[:2], units[2:]

    def outs(layer):
        return [
            pltpu.make_async_copy(gu.at[layer], ogu[layer], out_sem.at[2 * layer]),
            pltpu.make_async_copy(dd.at[layer], od[layer], out_sem.at[2 * layer + 1]),
        ]

    @pl.when(step == 0)
    def _():
        for layer in range(layers):
            for k in range(0, ff, LANE):
                gu[layer, x, y, :, 2 * k : 2 * k + LANE] = wg_ref[layer, :, k : k + LANE]
                gu[layer, x, y, :, 2 * k + LANE : 2 * k + 2 * LANE] = wu_ref[layer, :, k : k + LANE]
            dd[layer, x, y] = wd_ref[layer]
        entry_barrier(neighbours() + [partner])
        for letter in "ABCDE":
            for unit in first:
                unit.advance(letter, partner)
        for unit in rest:
            unit.advance("A", partner)
        for unit in first:
            unit.finish(partner)
        for copy in outs(0):
            copy.start()
        r = dd.shape[3]
        for d in range(SIDE * SIDE):
            wide_d[r * d : r * (d + 1)] = dd[0, d // SIDE, d % SIDE].astype(F32)
        wd0[...] = wide_d[...].astype(BF)

    for when, letter in ((1, "B"), (2, "C"), (4, "D"), (6, "E")):

        @pl.when(step == when)
        def _():
            for unit in rest:
                unit.advance(letter, partner)

    h = x_ref[...]
    wide = h.astype(F32)
    a = (wide * inverse_rms(wide)).astype(BF)
    total = jnp.zeros(h.shape, F32)
    w = gu.at[0]
    for j in range(0, ff, 2 * LANE):
        c = min(2 * LANE, ff - j)
        both = dot(a, w[:, :, :, 2 * j : 2 * (j + c)].reshape(h.shape[1], 2 * c))
        products = []
        for k in range(0, c, LANE):
            g, u = both[:, 2 * k : 2 * k + LANE], both[:, 2 * k + LANE : 2 * k + 2 * LANE]
            products.append((g * jax.nn.sigmoid(g) * u).astype(BF))
        total += dot(jnp.concatenate(products, 1), wd0[j : j + c, :])
    h_ref[...] = h + total.astype(BF)

    @pl.when(step == steps - 1)
    def _():
        for unit in rest:
            unit.finish(partner)
        for layer in range(1, layers):
            for copy in outs(layer):
                copy.start()
        for unit in units:
            unit.drain(partner)
        for layer in range(layers):
            for copy in outs(layer):
                copy.wait()


def forward(x, wg, wu, wd):
    tokens, d = x.shape
    layers, rows, ff = wg.shape
    rows_d = wd.shape[1]
    whole = lambda a: pl.BlockSpec(a.shape, lambda i: (0,) * a.ndim)
    h, *full = pl.pallas_call(
        functools.partial(forward_kernel, layers),
        grid=(tokens // TILE,),
        in_specs=[whole(wg), whole(wu), whole(wd), pl.BlockSpec((TILE, d), lambda i: (i, 0))],
        out_specs=[pl.BlockSpec((TILE, d), lambda i: (i, 0))] + [pl.BlockSpec(memory_space=pl.ANY)] * (2 * layers),
        out_shape=[jax.ShapeDtypeStruct((tokens, d), BF)]
        + [jax.ShapeDtypeStruct((SIDE, SIDE, rows, 2 * ff), BF)] * layers
        + [jax.ShapeDtypeStruct((SIDE, SIDE, rows_d, d), BF)] * layers,
        scratch_shapes=[
            pltpu.VMEM((layers, SIDE, SIDE, rows, 2 * ff), BF),
            pltpu.VMEM((layers, SIDE, SIDE, rows_d, d), BF),
            pltpu.VMEM((ff, d), F32),
            pltpu.VMEM((ff, d), BF),
            pltpu.SemaphoreType.DMA((2 * layers * 17,)),
            pltpu.SemaphoreType.DMA((2 * layers * 17,)),
            pltpu.SemaphoreType.DMA((2 * layers,)),
        ],
        compiler_params=pltpu.CompilerParams(collective_id=1, has_side_effects=True, vmem_limit_bytes=60 * 2**20),
    )(wg, wu, wd, x)
    return h, [one.reshape(d, 2 * ff) for one in full[:layers]], [one.reshape(ff, d) for one in full[layers:]]


def layer_kernel(through, h_ref, dy_ref, wgu_ref, wd_ref, *refs):
    if through:
        dh_ref, *refs = refs
    dwgu_ref, dwd_ref, accgu, accd, dgu, prod = refs
    step, steps = pl.program_id(0), pl.num_programs(0)
    ff = wd_ref.shape[0]

    @pl.when(step == 0)
    def _():
        accgu[...] = jnp.zeros_like(accgu)
        accd[...] = jnp.zeros_like(accd)

    wide = h_ref[...].astype(F32)
    scale = inverse_rms(wide)
    a = (wide * scale).astype(BF)
    dy = dy_ref[...]
    for j in range(0, ff, 2 * LANE):
        c = min(2 * LANE, ff - j)
        both = dot(a, wgu_ref[:, 2 * j : 2 * (j + c)])
        by = dot(dy, wd_ref[j : j + c, :], 1, 1).astype(BF).astype(F32)
        for k in range(0, c, LANE):
            g, u, b = both[:, 2 * k : 2 * k + LANE], both[:, 2 * k + LANE : 2 * k + 2 * LANE], by[:, k : k + LANE]
            s = jax.nn.sigmoid(g)
            silu = g * s
            at = j + k
            prod[:, at : at + LANE] = (silu * u).astype(BF)
            dgu[:, 2 * at : 2 * at + LANE] = (b * u * (s + silu * (1 - s))).astype(BF)
            dgu[:, 2 * at + LANE : 2 * at + 2 * LANE] = (b * silu).astype(BF)
    if through:
        da = dot(dgu[...], wgu_ref[...], 1, 1)
        back = scale * (da - wide * (scale * scale * jnp.mean(da * wide, -1, keepdims=True)))
        dh_ref[...] = dy + back.astype(BF)
    accgu[...] += dot(a, dgu[...], 0, 0)
    accd[...] += dot(prod[...], dy, 0, 0)

    @pl.when(step == steps - 1)
    def _():
        r, q = dwgu_ref.shape[2], dwd_ref.shape[2]
        for d in range(SIDE * SIDE):
            dwgu_ref[d // SIDE, d % SIDE] = accgu[r * d : r * (d + 1)].astype(BF)
            dwd_ref[d // SIDE, d % SIDE] = accd[q * d : q * (d + 1)].astype(BF)


def layer_back(through, h, dy, wgu, wd):
    tokens, d = h.shape
    ff = wd.shape[0]
    n = SIDE * SIDE
    tile = pl.BlockSpec((TILE, d), lambda i: (i, 0))
    whole = lambda shape: pl.BlockSpec(shape, lambda i: (0,) * len(shape))
    gu, dd = (SIDE, SIDE, d // n, 2 * ff), (SIDE, SIDE, ff // n, d)
    out_specs, out_shape = [whole(gu), whole(dd)], [jax.ShapeDtypeStruct(gu, BF), jax.ShapeDtypeStruct(dd, BF)]
    if through:
        out_specs, out_shape = [tile] + out_specs, [jax.ShapeDtypeStruct((tokens, d), BF)] + out_shape
    return pl.pallas_call(
        functools.partial(layer_kernel, through),
        grid=(tokens // TILE,),
        in_specs=[tile, tile, whole(wgu.shape), whole(wd.shape)],
        out_specs=out_specs,
        out_shape=out_shape,
        scratch_shapes=[
            pltpu.VMEM((d, 2 * ff), F32),
            pltpu.VMEM((ff, d), F32),
            pltpu.VMEM((TILE, 2 * ff), BF),
            pltpu.VMEM((TILE, ff), BF),
        ],
        compiler_params=pltpu.CompilerParams(vmem_limit_bytes=60 * 2**20),
    )(h, dy, wgu, wd)


class Scatter:
    def __init__(self, terms, bufs, send, recv, base):
        self.terms, self.send, self.recv, self.base = terms, send, recv, base
        self.a, self.b, self.sums, self.out, self.c, self.d = bufs
        self.half = terms.shape[-1] // 2
        r = terms.shape[2]
        if r % 32 == 0:
            self.parts = [(pl.ds(0, r // 2), slice(None)), (pl.ds(r // 2, r // 2), slice(None))]
        else:
            q = self.half // 2
            self.parts = [(slice(None), pl.ds(0, q)), (slice(None), pl.ds(q, q))]

    @staticmethod
    def scratch(rows, columns):
        half = columns // 2
        return [
            pltpu.VMEM((2, 2, SIDE // 2, rows, half), BF),
            pltpu.VMEM((2, 2, SIDE, rows, half), BF),
            pltpu.VMEM((2, SIDE, rows, half), F32),
            pltpu.VMEM((2, SIDE, rows, half), BF),
            pltpu.VMEM((2, rows, half), BF),
            pltpu.VMEM((2, 2, rows, half), BF),
        ]

    def index(self, which, first, second):
        cols = pl.ds(which * self.half, self.half)
        return (second, first, slice(None), cols) if which == 0 else (first, second, slice(None), cols)

    def copies(self, step):
        out = []
        for which, order in enumerate("yx"):
            i1, i2 = ring_places(order)
            for side in range(2):
                by = 1 - 2 * side
                if step == "A":
                    src = self.terms.at[self.index(which, shifted(i1, 2), pl.ds(side * (SIDE // 2), SIDE // 2))]
                    dst = self.a.at[which, side]
                elif step == "B":
                    src = self.terms.at[self.index(which, shifted(i1, by), slice(None))]
                    dst = self.b.at[which, side]
                elif step == "C":
                    rows, cols = self.parts[side]
                    src = self.out.at[which, shifted(i2, 2), rows, cols]
                    dst = self.c.at[which, rows, cols]
                else:
                    src = self.out.at[which, shifted(i2, by)]
                    dst = self.d.at[which, side]
                number = self.base + STEPS.index(step) * 4 + which * 2 + side
                out.append(
                    pltpu.make_async_remote_copy(
                        src_ref=src,
                        dst_ref=dst,
                        send_sem=self.send.at[number],
                        recv_sem=self.recv.at[number],
                        device_id=along(order, by, step in "CD"),
                        device_id_type=MESH,
                    )
                )
        return out

    def advance(self, step):
        if step != "A":
            for copy in self.copies("ABCD"["ABCDE".index(step) - 1]):
                copy.wait_recv()
        for which, order in enumerate("yx"):
            i1, i2 = ring_places(order)
            if step == "B":
                for side in range(2):
                    for k in range(SIDE // 2):
                        at = self.index(which, shifted(i1, 1 - 2 * side), side * (SIDE // 2) + k)
                        self.terms[at] = (self.terms[at].astype(F32) + self.a[which, side, k].astype(F32)).astype(BF)
            elif step == "C":

                def own(k, _):
                    mine = self.terms[self.index(which, i1, k)].astype(F32)
                    self.sums[which, k] = mine + self.b[which, 0, k].astype(F32) + self.b[which, 1, k].astype(F32)
                    return 0

                lax.fori_loop(0, SIDE, own, 0)
                far = shifted(i2, 2)
                self.out[which, far] = self.sums[which, far].astype(BF)
            elif step == "D":
                for side in range(2):
                    near = shifted(i2, 1 - 2 * side)
                    for part in range(2):
                        at = self.parts[part]
                        value = self.sums[(which, near) + at]
                        if part == side:
                            value = value + self.c[(which,) + at].astype(F32)
                        self.out[(which, near) + at] = value.astype(BF)
        if step != "E":
            for copy in self.copies(step):
                copy.start()

    def result(self):
        halves = []
        for which, order in enumerate("yx"):
            _, i2 = ring_places(order)
            total = self.sums[which, i2] + self.d[which, 0].astype(F32) + self.d[which, 1].astype(F32)
            halves.append(total.astype(BF))
        return halves

    def drain(self):
        for step in STEPS:
            for copy in self.copies(step):
                copy.wait_send()


def sum_everywhere(value, mine, theirs, send, recv, base):
    for which, order in enumerate("yx"):
        mine[which] = jnp.broadcast_to(value, mine.shape[1:])
        copies = [
            pltpu.make_async_remote_copy(
                src_ref=mine.at[which],
                dst_ref=theirs.at[which, by - 1],
                send_sem=send.at[base + which * 3 + by - 1],
                recv_sem=recv.at[base + which * 3 + by - 1],
                device_id=along(order, by),
                device_id_type=MESH,
            )
            for by in range(1, SIDE)
        ]
        for copy in copies:
            copy.start()
        for copy in copies:
            copy.wait()
        value = value + theirs[which, 0][:1, :1] + theirs[which, 1][:1, :1] + theirs[which, 2][:1, :1]
    return value


def reduce_kernel(layers, *refs):
    gus, dds, (rg, ru, rd, total), refs = refs[:layers], refs[layers : 2 * layers], refs[2 * layers : 2 * layers + 4], refs[2 * layers + 4 :]
    terms, refs = refs[: 2 * layers], refs[2 * layers :]
    bufs, (mine, theirs, send, recv, load) = refs[: 12 * layers], refs[12 * layers :]
    units = [Scatter(terms[n], bufs[6 * n : 6 * n + 6], send, recv, 16 * n) for n in range(2 * layers)]
    sources = [one for layer in reversed(range(layers)) for one in (gus[layer], dds[layer])]
    loads = [pltpu.make_async_copy(source, term, load.at[n]) for n, (source, term) in enumerate(zip(sources, terms, strict=True))]
    for copy in loads:
        copy.start()
    entry_barrier(neighbours() + [along("y", 2), along("x", 2)])
    for copy, unit in zip(loads, units, strict=True):
        copy.wait()
        unit.advance("A")
    for letter in "BCDE":
        for unit in units:
            unit.advance(letter)
    squares = jnp.zeros((1, 1), F32)
    for n, unit in enumerate(units):
        layer = layers - 1 - n // 2
        for which, half in enumerate(unit.result()):
            wide = half.astype(F32)
            squares += jnp.sum(wide * wide, keepdims=True)
            width = half.shape[1]
            if n % 2:
                rd[layer, :, which * width : (which + 1) * width] = half
            else:
                for k in range(0, width, LANE):
                    block = (which * width + k) // LANE
                    out = (rg, ru)[block % 2]
                    out[layer, :, block // 2 * LANE : (block // 2 + 1) * LANE] = half[:, k : k + LANE]
    total[...] = jnp.broadcast_to(sum_everywhere(squares, mine, theirs, send, recv, 16 * len(units)), total.shape)
    for unit in units:
        unit.drain()


def reduced(gus, dds):
    layers = len(gus)
    rows, ff = gus[0].shape[2], gus[0].shape[3] // 2
    rows_d, d = dds[0].shape[2:]
    shapes = [one.shape for _ in range(layers) for one in (gus[0], dds[0])]
    scratch = [pltpu.VMEM(shape, BF) for shape in shapes]
    for shape in shapes:
        scratch += Scatter.scratch(shape[2], shape[3])
    n = 16 * len(shapes) + 6
    return pl.pallas_call(
        functools.partial(reduce_kernel, layers),
        in_specs=[pl.BlockSpec(memory_space=pl.ANY)] * (2 * layers),
        out_specs=[pl.BlockSpec(memory_space=pltpu.VMEM)] * 4,
        out_shape=[
            jax.ShapeDtypeStruct((layers, rows, ff), BF),
            jax.ShapeDtypeStruct((layers, rows, ff), BF),
            jax.ShapeDtypeStruct((layers, rows_d, d), BF),
            jax.ShapeDtypeStruct((8, LANE), F32),
        ],
        scratch_shapes=scratch
        + [
            pltpu.VMEM((2, 8, LANE), F32),
            pltpu.VMEM((2, SIDE - 1, 8, LANE), F32),
            pltpu.SemaphoreType.DMA((n,)),
            pltpu.SemaphoreType.DMA((n,)),
            pltpu.SemaphoreType.DMA((len(shapes),)),
        ],
        compiler_params=pltpu.CompilerParams(collective_id=2, has_side_effects=True, vmem_limit_bytes=60 * 2**20),
    )(*gus, *dds)


def adamw(w, m, v, g):
    m = 0.9 * m + 0.1 * g
    v = 0.95 * v + 0.05 * g * g
    step = m * lax.rsqrt(v + 1e-8) + 0.1 * w
    return (w - 0.02 * step).astype(jnp.bfloat16), m, v


def solution(mesh):
    group = mesh.shape["dp"]

    def step(x, dy, *arrays):
        weights, m, v = (arrays[i : i + 3] for i in (0, 3, 6))
        h0, by1 = x[0], dy[0]
        h1, wgu, wd = forward(h0, *weights)
        by0, gu1, dd1 = layer_back(True, h1, by1, wgu[1], wd[1])
        gu0, dd0 = layer_back(False, h0, by0, wgu[0], wd[0])
        *gradients, total = reduced([gu0, gu1], [dd0, dd1])
        count = group * sum(g.size for g in gradients)
        factor = jnp.minimum(1.0, 0.5 * lax.rsqrt(total[0, 0] / count + 1e-30))
        new = [adamw(w.astype(F32), m, v, g.astype(F32) * factor) for w, m, v, g in zip(weights, m, v, gradients, strict=True)]
        return tuple(one[which] for which in range(3) for one in new)

    states, cut = P(("rep", "dp"), None, None), P(None, "dp", None)
    return jax.shard_map(
        step,
        mesh=mesh,
        in_specs=(states, states) + (cut,) * 9,
        out_specs=(P("rep", "dp", None),) * 9,
        check_vma=False,
    )
```

```python
import functools

import jax
import jax.numpy as jnp
from jax import lax
from jax.experimental import pallas as pl
from jax.experimental.pallas import tpu as pltpu
from jax.sharding import PartitionSpec as P

F32, BF = jnp.float32, jnp.bfloat16
MESH = pl.DeviceIdType.MESH
LANE = 128
TILE = 512
FORWARD_TILE = 1024
BACK_TILE = 1024
SIDE = 4
HOPS = (1, -1, 2)


def dot(a, b, ca=1, cb=0):
    return lax.dot_general(a, b, (((ca,), (cb,)), ((), ())), preferred_element_type=F32)


def inverse_rms(wide):
    return lax.rsqrt(jnp.mean(wide * wide, -1, keepdims=True) + 1e-6)


def place():
    me = lax.axis_index("dp")
    return me // SIDE, lax.rem(me, SIDE)


def others():
    return [along(order, by) for order in "yx" for by in HOPS]


def shifted(i, by):
    return lax.rem(i + by + SIDE, SIDE)


def along(order, by, second=False):
    x, y = place()
    if (order == "y") != second:
        return {"dp": x * SIDE + shifted(y, by)}
    return {"dp": shifted(x, by) * SIDE + y}


def ring_places(order):
    x, y = place()
    return (y, x) if order == "y" else (x, y)


def entry_barrier(peers):
    with jax.named_scope("entry"):
        barrier = pltpu.get_barrier_semaphore()
        for peer in peers:
            pl.semaphore_signal(barrier, inc=1, device_id=peer, device_id_type=MESH)
        pl.semaphore_wait(barrier, len(peers))


class Gather:
    def __init__(self, buf, core, cut, rows, send, recv, base, direct=False):
        self.steps = "ACE" if direct else "ABCDE"
        self.buf, self.core, self.send, self.recv, self.base = buf, core, send, recv, base
        half = buf.shape[-1] // 2
        self.half, self.rows, self.r = half, rows, buf.shape[-2]
        self.columns = {"y": (0, cut), "x": (cut, half - cut)}

    def at(self, order, first, second, rows=slice(None)):
        off, width = self.columns[order]
        cols = pl.ds(pl.multiple_of(self.core * self.half + off, LANE), width)
        a, b = (second, first) if order == "y" else (first, second)
        return self.buf.at[a, b, rows, cols]

    def copies(self, step):
        out = []
        for which, order in enumerate("yx"):
            i1, i2 = ring_places(order)
            hops = HOPS if self.steps == "ACE" else HOPS[:2]
            if step == "A":
                refs = [self.at(order, i1, i2)] * len(hops)
            elif step == "B":
                refs = [
                    self.at(order, shifted(i1, -1), i2, pl.ds(0, self.rows)),
                    self.at(order, shifted(i1, 1), i2, pl.ds(self.rows, self.r - self.rows)),
                ]
            elif step == "C":
                refs = [self.at(order, slice(None), i2)] * len(hops)
            else:
                refs = [
                    self.at(order, pl.ds(0, SIDE // 2), shifted(i2, -1)),
                    self.at(order, pl.ds(SIDE // 2, SIDE // 2), shifted(i2, 1)),
                ]
            for side, ref in enumerate(refs):
                number = self.base + self.steps.index(step) * 2 * len(hops) + which * len(hops) + side
                out.append(
                    pltpu.make_async_remote_copy(
                        src_ref=ref,
                        dst_ref=ref,
                        send_sem=self.send.at[number],
                        recv_sem=self.recv.at[number],
                        device_id=along(order, hops[side], step in "CD"),
                        device_id_type=MESH,
                    )
                )
        return out

    def across(self, partner):
        ref = self.buf.at[:, :, :, pl.ds(pl.multiple_of(self.core * self.half, LANE), self.half)]
        number = self.base + 16
        return pltpu.make_async_remote_copy(
            src_ref=ref, dst_ref=ref, send_sem=self.send.at[number], recv_sem=self.recv.at[number], device_id=partner, device_id_type=MESH
        )

    def advance(self, step, partner):
        if step != "A":
            with jax.named_scope(f"wait_{step}{self.base // 17}"):
                for copy in self.copies(self.steps[self.steps.index(step) - 1]):
                    copy.wait_recv()
        if step == "E":
            self.across(partner).start()
        else:
            for copy in self.copies(step):
                copy.start()

    def finish(self, partner):
        with jax.named_scope(f"wait_F{self.base // 17}"):
            self.across(partner).wait_recv()

    def drain(self, partner):
        for step in self.steps[:-1]:
            for copy in self.copies(step):
                copy.wait_send()
        self.across(partner).wait_send()


def pieces_of(ff):
    cuts = [0, 3 * LANE, 7 * LANE, ff]
    return list(zip(cuts[:-1], cuts[1:]))


def forward_kernel(layers, wg_ref, wu_ref, wd_ref, x_hbm, h_hbm, a_hbm, prod_hbm, *refs):
    (ogu, od), refs = (refs[:layers], refs[layers : 2 * layers]), refs[2 * layers :]
    ff = wg_ref.shape[2]
    pieces = pieces_of(ff)
    first, (later, dd, xv, a, prod, wide_d, wd0, send, recv, out_sem, h_sem, p_sem) = refs[: len(pieces)], refs[len(pieces) :]
    tokens, d = xv.shape
    tiles = tokens // FORWARD_TILE
    rep = lax.axis_index("rep")
    core = lax.rem(rep, 2)
    partner = {"rep": rep + 1 - 2 * core}
    x, y = place()
    x_load = pltpu.make_async_copy(x_hbm, xv, out_sem.at[0])
    x_load.start()

    def placed(buf, layer, start, stop):
        for k in range(start, stop, LANE):
            at = 2 * (k - start)
            buf[x, y, :, at : at + LANE] = wg_ref[layer, :, k : k + LANE]
            buf[x, y, :, at + LANE : at + 2 * LANE] = wu_ref[layer, :, k : k + LANE]

    bufs = list(first) + [dd.at[0]]
    for buf, (start, stop) in zip(first, pieces, strict=True):
        placed(buf, 0, start, stop)
    for layer in range(1, layers):
        placed(later.at[layer - 1], layer, 0, ff)
        bufs += [later.at[layer - 1], dd.at[layer]]
    for layer in range(layers):
        dd[layer, x, y] = wd_ref[layer]
    entry_barrier(others() + [partner])

    def unit_of(n, buf):
        quarter = (buf.shape[-1] // 4 + LANE - 1) // LANE * LANE
        return Gather(buf, core, quarter, 16 if buf.shape[2] % 32 == 0 else 48, send, recv, 17 * n, n == 0)

    units = [unit_of(n, buf) for n, buf in enumerate(bufs)]
    gus, down, rest = units[: len(pieces)], units[len(pieces)], units[len(pieces) + 1 :]
    one, two, three = gus

    def go(step, *those):
        for unit in those:
            unit.advance(step, partner)

    go("A", *gus, down)
    x_load.wait()

    def norm(t, _):
        rows = pl.ds(pl.multiple_of(t * FORWARD_TILE, FORWARD_TILE), FORWARD_TILE)
        wide = xv[rows].astype(F32)
        a[rows] = (wide * inverse_rms(wide)).astype(BF)
        return 0

    with jax.named_scope("norm"):
        lax.fori_loop(0, tiles, norm, 0)
    go("C", one)
    go("B", two, three, down)
    go("C", two)
    go("E", one)
    slots = [
        {2: [("D", [two]), ("C", [three])], 4: [("C", [down])], 6: [("E", [two]), ("D", [three]), ("A", rest)]},
        {0: [("D", [down])], 2: [("E", [three]), ("B", rest)], 4: [("E", [down]), ("C", rest)]},
        {},
    ]
    for unit, buf, (start, stop), slot in zip(gus, first, pieces, slots, strict=True):
        unit.finish(partner)

        def products(t, _):
            for when, actions in slot.items():

                @pl.when(t == when * tiles // 8)
                def _():
                    for step, those in actions:
                        go(step, *those)

            rows = pl.ds(pl.multiple_of(t * FORWARD_TILE, FORWARD_TILE), FORWARD_TILE)
            at = a[rows]
            for j in range(start, stop, 2 * LANE):
                c = min(2 * LANE, stop - j)
                w = buf[:, :, :, 2 * (j - start) : 2 * (j - start + c)].reshape(d, 2 * c)
                both = dot(at, w)
                for k in range(0, c, LANE):
                    g, u = both[:, 2 * k : 2 * k + LANE], both[:, 2 * k + LANE : 2 * k + 2 * LANE]
                    prod[rows, j + k : j + k + LANE] = (g * jax.nn.sigmoid(g) * u).astype(BF)
            return 0

        with jax.named_scope(f"products_{start}"):
            lax.fori_loop(0, tiles, products, 0)

    def gu_out(n):
        start, stop = pieces[n]
        return pltpu.make_async_copy(first[n], ogu[0].at[:, :, :, 2 * start : 2 * stop], out_sem.at[n])

    a_out = pltpu.make_async_copy(a, a_hbm, h_sem.at[tiles])
    a_out.start()
    outs = [gu_out(n) for n in range(len(pieces))] + [pltpu.make_async_copy(dd.at[0], od[0], out_sem.at[len(pieces)])]
    for layer in range(1, layers):
        n = len(outs)
        outs.append(pltpu.make_async_copy(later.at[layer - 1], ogu[layer], out_sem.at[n]))
        outs.append(pltpu.make_async_copy(dd.at[layer], od[layer], out_sem.at[n + 1]))
    down.finish(partner)
    for copy in outs[: len(pieces) + 1]:
        copy.start()
    r = dd.shape[3]
    for n in range(SIDE * SIDE):
        wide_d[r * n : r * (n + 1)] = dd[0, n // SIDE, n % SIDE].astype(F32)
    wd0[...] = wide_d[...].astype(BF)

    def tile_outs(t):
        rows = pl.ds(pl.multiple_of(t * FORWARD_TILE, FORWARD_TILE), FORWARD_TILE)
        return [pltpu.make_async_copy(xv.at[rows], h_hbm.at[rows], h_sem.at[t]), pltpu.make_async_copy(prod.at[rows], prod_hbm.at[rows], p_sem.at[t])]

    def close(t, _):
        for when, step in ((0, "D"), (tiles // 2, "E")):

            @pl.when(t == when)
            def _():
                go(step, *rest)

        rows = pl.ds(pl.multiple_of(t * FORWARD_TILE, FORWARD_TILE), FORWARD_TILE)
        xv[rows] = xv[rows] + dot(prod[rows], wd0[...]).astype(BF)
        for copy in tile_outs(t):
            copy.start()
        return 0

    with jax.named_scope("close"):
        lax.fori_loop(0, tiles, close, 0)
    for unit in rest:
        unit.finish(partner)
    for copy in outs[len(pieces) + 1 :]:
        copy.start()
    for unit in units:
        unit.drain(partner)

    def closed(t, _):
        for copy in tile_outs(t):
            copy.wait()
        return 0

    with jax.named_scope("out_wait"):
        lax.fori_loop(0, tiles, closed, 0)
        for copy in outs + [a_out]:
            copy.wait()


def forward(x, wg, wu, wd):
    tokens, d = x.shape
    layers, rows, ff = wg.shape
    rows_d = wd.shape[1]
    pieces = pieces_of(ff)
    n = 17 * (len(pieces) + 2 * layers - 1)
    anywhere = pl.BlockSpec(memory_space=pl.ANY)
    h, a, prod, *full = pl.pallas_call(
        functools.partial(forward_kernel, layers),
        in_specs=[pl.BlockSpec(memory_space=pltpu.VMEM)] * 3 + [anywhere],
        out_specs=[anywhere] * (3 + 2 * layers),
        out_shape=[jax.ShapeDtypeStruct((tokens, d), BF)] * 2
        + [jax.ShapeDtypeStruct((tokens, ff), BF)]
        + [jax.ShapeDtypeStruct((SIDE, SIDE, rows, 2 * ff), BF)] * layers
        + [jax.ShapeDtypeStruct((SIDE, SIDE, rows_d, d), BF)] * layers,
        scratch_shapes=[pltpu.VMEM((SIDE, SIDE, rows, 2 * (stop - start)), BF) for start, stop in pieces]
        + [
            pltpu.VMEM((layers - 1, SIDE, SIDE, rows, 2 * ff), BF),
            pltpu.VMEM((layers, SIDE, SIDE, rows_d, d), BF),
            pltpu.VMEM((tokens, d), BF),
            pltpu.VMEM((tokens, d), BF),
            pltpu.VMEM((tokens, ff), BF),
            pltpu.VMEM((ff, d), F32),
            pltpu.VMEM((ff, d), BF),
            pltpu.SemaphoreType.DMA((n,)),
            pltpu.SemaphoreType.DMA((n,)),
            pltpu.SemaphoreType.DMA((len(pieces) + 2 * layers - 1,)),
            pltpu.SemaphoreType.DMA((tokens // FORWARD_TILE + 1,)),
            pltpu.SemaphoreType.DMA((tokens // FORWARD_TILE,)),
        ],
        compiler_params=pltpu.CompilerParams(collective_id=1, has_side_effects=True, vmem_limit_bytes=60 * 2**20),
    )(wg, wu, wd, x)
    return h, a, prod, [one.reshape(d, 2 * ff) for one in full[:layers]], [one.reshape(ff, d) for one in full[layers:]]


def hidden_back(both, by):
    g, u, b = both[:, :LANE], both[:, LANE:], by.astype(BF).astype(F32)
    s = jax.nn.sigmoid(g)
    silu = g * s
    return (b * u * (s + silu * (1 - s))).astype(BF), (b * silu).astype(BF), (silu * u).astype(BF)


def layer_kernel(h_ref, dy_ref, wgu_ref, wd_ref, dh_ref, dwgu_ref, dwd_ref, accgu, accd, dgu, prod):
    step, steps = pl.program_id(0), pl.num_programs(0)
    ff = wd_ref.shape[0]

    @pl.when(step == 0)
    def _():
        accgu[...] = jnp.zeros_like(accgu)
        accd[...] = jnp.zeros_like(accd)

    wide = h_ref[...].astype(F32)
    scale = inverse_rms(wide)
    a = (wide * scale).astype(BF)
    dy = dy_ref[...]
    for j in range(0, ff, 2 * LANE):
        c = min(2 * LANE, ff - j)
        both = dot(a, wgu_ref[:, 2 * j : 2 * (j + c)])
        by = dot(dy, wd_ref[j : j + c, :], 1, 1)
        for k in range(0, c, LANE):
            at = j + k
            dg, du, product = hidden_back(both[:, 2 * k : 2 * (k + LANE)], by[:, k : k + LANE])
            prod[:, at : at + LANE] = product
            dgu[:, 2 * at : 2 * at + LANE] = dg
            dgu[:, 2 * at + LANE : 2 * at + 2 * LANE] = du
    da = dot(dgu[...], wgu_ref[...], 1, 1)
    back = scale * (da - wide * (scale * scale * jnp.mean(da * wide, -1, keepdims=True)))
    dh_ref[...] = dy + back.astype(BF)
    accgu[...] += dot(a, dgu[...], 0, 0)
    accd[...] += dot(prod[...], dy, 0, 0)

    @pl.when(step == steps - 1)
    def _():
        r, q = dwgu_ref.shape[2], dwd_ref.shape[2]
        for d in range(SIDE * SIDE):
            dwgu_ref[d // SIDE, d % SIDE] = accgu[r * d : r * (d + 1)].astype(BF)
            dwd_ref[d // SIDE, d % SIDE] = accd[q * d : q * (d + 1)].astype(BF)


def layer_back(h, dy, wgu, wd):
    tokens, d = h.shape
    ff = wd.shape[0]
    n = SIDE * SIDE
    tile = pl.BlockSpec((TILE, d), lambda i: (i, 0))
    whole = lambda shape: pl.BlockSpec(shape, lambda i: (0,) * len(shape))
    gu, dd = (SIDE, SIDE, d // n, 2 * ff), (SIDE, SIDE, ff // n, d)
    return pl.pallas_call(
        layer_kernel,
        grid=(tokens // TILE,),
        in_specs=[tile, tile, whole(wgu.shape), whole(wd.shape)],
        out_specs=[tile, whole(gu), whole(dd)],
        out_shape=[jax.ShapeDtypeStruct((tokens, d), BF), jax.ShapeDtypeStruct(gu, BF), jax.ShapeDtypeStruct(dd, BF)],
        scratch_shapes=[
            pltpu.VMEM((d, 2 * ff), F32),
            pltpu.VMEM((ff, d), F32),
            pltpu.VMEM((TILE, 2 * ff), BF),
            pltpu.VMEM((TILE, ff), BF),
        ],
        compiler_params=pltpu.CompilerParams(vmem_limit_bytes=60 * 2**20),
    )(h, dy, wgu, wd)


class Scatter:
    def __init__(self, terms, bufs, send, recv, base):
        self.terms, self.send, self.recv, self.base = terms, send, recv, base
        self.a, self.b, self.sums, self.out, self.c, self.d = bufs
        self.half = terms.shape[-1] // 2
        r = terms.shape[2]
        if r % 32 == 0:
            self.parts = [(pl.ds(0, r // 2), slice(None)), (pl.ds(r // 2, r // 2), slice(None))]
        else:
            q = self.half // 2
            self.parts = [(slice(None), pl.ds(0, q)), (slice(None), pl.ds(q, q))]

    @staticmethod
    def scratch(rows, columns):
        half = columns // 2
        return [
            pltpu.VMEM((2, 2, SIDE // 2, rows, half), BF),
            pltpu.VMEM((2, 2, SIDE, rows, half), BF),
            pltpu.VMEM((2, SIDE, rows, half), F32),
            pltpu.VMEM((2, SIDE, rows, half), BF),
            pltpu.VMEM((2, rows, half), BF),
            pltpu.VMEM((2, 2, rows, half), BF),
        ]

    def index(self, which, first, second):
        cols = pl.ds(which * self.half, self.half)
        return (second, first, slice(None), cols) if which == 0 else (first, second, slice(None), cols)

    def copies(self, step):
        out = []
        for which, order in enumerate("yx"):
            i1, i2 = ring_places(order)
            for side in range(2):
                by = 1 - 2 * side
                if step == "A":
                    src = self.terms.at[self.index(which, shifted(i1, 2), pl.ds(side * (SIDE // 2), SIDE // 2))]
                    dst = self.a.at[which, side]
                elif step == "B":
                    src = self.terms.at[self.index(which, shifted(i1, by), slice(None))]
                    dst = self.b.at[which, side]
                elif step == "C":
                    rows, cols = self.parts[side]
                    src = self.out.at[which, shifted(i2, 2), rows, cols]
                    dst = self.c.at[which, rows, cols]
                else:
                    src = self.out.at[which, shifted(i2, by)]
                    dst = self.d.at[which, side]
                number = self.base + "ABCD".index(step) * 4 + which * 2 + side
                out.append(
                    pltpu.make_async_remote_copy(
                        src_ref=src,
                        dst_ref=dst,
                        send_sem=self.send.at[number],
                        recv_sem=self.recv.at[number],
                        device_id=along(order, by, step in "CD"),
                        device_id_type=MESH,
                    )
                )
        return out

    def advance(self, step):
        if step != "A":
            with jax.named_scope(f"wait_{step}{self.base // 16}"):
                for copy in self.copies("ABCD"["ABCDE".index(step) - 1]):
                    copy.wait_recv()
        for which, order in enumerate("yx"):
            i1, i2 = ring_places(order)
            if step == "B":
                for side in range(2):
                    for k in range(SIDE // 2):
                        at = self.index(which, shifted(i1, 1 - 2 * side), side * (SIDE // 2) + k)
                        self.terms[at] = (self.terms[at].astype(F32) + self.a[which, side, k].astype(F32)).astype(BF)
            elif step == "C":

                def own(k, _):
                    mine = self.terms[self.index(which, i1, k)].astype(F32)
                    self.sums[which, k] = mine + self.b[which, 0, k].astype(F32) + self.b[which, 1, k].astype(F32)
                    return 0

                lax.fori_loop(0, SIDE, own, 0)
                far = shifted(i2, 2)
                self.out[which, far] = self.sums[which, far].astype(BF)
            elif step == "D":
                for side in range(2):
                    near = shifted(i2, 1 - 2 * side)
                    for part in range(2):
                        at = self.parts[part]
                        value = self.sums[(which, near) + at]
                        if part == side:
                            value = value + self.c[(which,) + at].astype(F32)
                        self.out[(which, near) + at] = value.astype(BF)
        if step != "E":
            for copy in self.copies(step):
                copy.start()

    def result(self):
        halves = []
        for which, order in enumerate("yx"):
            _, i2 = ring_places(order)
            total = self.sums[which, i2] + self.d[which, 0].astype(F32) + self.d[which, 1].astype(F32)
            halves.append(total.astype(BF))
        return halves

    def drain(self):
        for step in "ABCD":
            for copy in self.copies(step):
                copy.wait_send()


class DirectScatter(Scatter):
    def __init__(self, terms, bufs, send, recv, base):
        self.terms, self.send, self.recv, self.base = terms, send, recv, base
        self.b, self.sums, self.out, self.d = bufs
        self.half = terms.shape[-1] // 2

    @staticmethod
    def scratch(rows, columns):
        half = columns // 2
        return [
            pltpu.VMEM((2, len(HOPS), SIDE, rows, half), BF),
            pltpu.VMEM((2, SIDE, rows, half), F32),
            pltpu.VMEM((2, SIDE, rows, half), BF),
            pltpu.VMEM((2, len(HOPS), rows, half), BF),
        ]

    def copies(self, step):
        out = []
        for which, order in enumerate("yx"):
            i1, i2 = ring_places(order)
            for k, by in enumerate(HOPS):
                if step == "A":
                    src, dst = self.terms.at[self.index(which, shifted(i1, by), slice(None))], self.b.at[which, k]
                else:
                    src, dst = self.out.at[which, shifted(i2, by)], self.d.at[which, k]
                number = self.base + (step == "C") * 6 + which * 3 + k
                out.append(
                    pltpu.make_async_remote_copy(
                        src_ref=src,
                        dst_ref=dst,
                        send_sem=self.send.at[number],
                        recv_sem=self.recv.at[number],
                        device_id=along(order, by, step == "C"),
                        device_id_type=MESH,
                    )
                )
        return out

    def advance(self, step):
        if step != "A":
            with jax.named_scope(f"wait_{step}{self.base // 16}"):
                for copy in self.copies("A" if step == "C" else "C"):
                    copy.wait_recv()
        if step == "C":
            for which, order in enumerate("yx"):
                i1, _ = ring_places(order)
                for k in range(SIDE):
                    total = self.terms[self.index(which, i1, k)].astype(F32)
                    for n in range(len(HOPS)):
                        total += self.b[which, n, k].astype(F32)
                    self.sums[which, k] = total
                    self.out[which, k] = total.astype(BF)
        if step != "E":
            for copy in self.copies(step):
                copy.start()

    def result(self):
        halves = []
        for which, order in enumerate("yx"):
            _, i2 = ring_places(order)
            total = self.sums[which, i2]
            for n in range(len(HOPS)):
                total += self.d[which, n].astype(F32)
            halves.append(total.astype(BF))
        return halves

    def drain(self):
        for step in "AC":
            for copy in self.copies(step):
                copy.wait_send()


def sum_everywhere(value, mine, theirs, send, recv, base):
    for which, order in enumerate("yx"):
        mine[which] = jnp.broadcast_to(value, mine.shape[1:])
        copies = [
            pltpu.make_async_remote_copy(
                src_ref=mine.at[which],
                dst_ref=theirs.at[which, by - 1],
                send_sem=send.at[base + which * 3 + by - 1],
                recv_sem=recv.at[base + which * 3 + by - 1],
                device_id=along(order, by),
                device_id_type=MESH,
            )
            for by in range(1, SIDE)
        ]
        with jax.named_scope(f"squares_{order}"):
            for copy in copies:
                copy.start()
            for copy in copies:
                copy.wait()
        value = value + theirs[which, 0][:1, :1] + theirs[which, 1][:1, :1] + theirs[which, 2][:1, :1]
    return value


def chunks_of(ff):
    cuts = [0, 4 * LANE, 8 * LANE, ff - LANE, ff]
    return list(zip(cuts[:-1], cuts[1:]))


def kinds_of(units):
    return [Scatter] * (units - 2) + [DirectScatter] * 2


def back_kernel(chunks, a_hbm, dh_hbm, wgu_hbm, wd_hbm, prod_hbm, gu_hbm, dd_hbm, rg, ru, rd, total, *refs):
    n_units = 3 + len(chunks)
    terms, refs = refs[:n_units], refs[n_units:]
    units = []
    for n, kind in enumerate(kinds_of(n_units)):
        count = len(kind.scratch(1, 2))
        units.append((kind, terms[n], refs[:count], 16 * n))
        refs = refs[count:]
    a, dh, wgu, wd, pbuf, accd, accg, dgu, mine, theirs, send, recv, load, p_sem = refs
    tokens, d = a.shape
    tiles = tokens // BACK_TILE
    units = [kind(term, bufs, send, recv, base) for kind, term, bufs, base in units]
    gu1, dd1, dd0, *parts = units
    pairs = [(gu_hbm, terms[0]), (dd_hbm, terms[1]), (dh_hbm, dh), (a_hbm, a), (wgu_hbm, wgu), (wd_hbm, wd)]
    loads = [pltpu.make_async_copy(source, to, load.at[n]) for n, (source, to) in enumerate(pairs)]
    rows_of = lambda t: pl.ds(pl.multiple_of(t * BACK_TILE, BACK_TILE), BACK_TILE)
    prod_load = lambda t: pltpu.make_async_copy(prod_hbm.at[rows_of(t)], pbuf.at[lax.rem(t, 2)], p_sem.at[lax.rem(t, 2)])
    for copy in loads[:3]:
        copy.start()
    prod_load(0).start()
    entry_barrier(others())
    for copy, unit in zip(loads[:2], units[:2], strict=True):
        copy.wait()
        unit.advance("A")
    loads[2].wait()
    accd[...] = jnp.zeros_like(accd)

    def down(t, _):
        @pl.when(t + 1 < tiles)
        def _():
            prod_load(t + 1).start()

        @pl.when(t == 0)
        def _():
            for copy in loads[3:]:
                copy.start()

        rows = rows_of(t)
        prod_load(t).wait()
        accd[...] += dot(pbuf[lax.rem(t, 2)], dh[rows], 0, 0)
        return 0

    with jax.named_scope("down"):
        lax.fori_loop(0, tiles, down, 0)
    q = terms[2].shape[2]
    for n in range(SIDE * SIDE):
        terms[2][n // SIDE, n % SIDE] = accd[q * n : q * (n + 1)].astype(BF)
    gu1.advance("B")
    for copy in loads[3:]:
        copy.wait()
    one, two, three, four = parts
    slots = [
        {4: [(dd1, "B"), (dd0, "A")], 6: [(gu1, "C")]},
        {0: [(one, "A"), (gu1, "D")], 2: [(dd1, "C"), (dd0, "B")], 4: [(one, "B")], 6: [(dd1, "D"), (dd0, "C")]},
        {0: [(two, "A")], 2: [(dd0, "D"), (one, "C")], 4: [(two, "B")], 6: [(one, "D")]},
        {0: [(three, "A")], 4: [(two, "C")]},
    ]
    for (start, stop), term, slot in zip(chunks, terms[3:], slots, strict=True):
        width = 2 * (stop - start)
        accg[:, :width] = jnp.zeros((d, width), F32)

        def chunk(t, _):
            for when, actions in slot.items():

                @pl.when(t == when * tiles // 8)
                def _():
                    for unit, step in actions:
                        unit.advance(step)

            rows = rows_of(t)
            at, by = a[rows], dh[rows]
            for j in range(start, stop, 2 * LANE):
                c = min(2 * LANE, stop - j)
                both = dot(at, wgu[:, 2 * j : 2 * (j + c)])
                back = dot(by, wd[j : j + c, :], 1, 1)
                for k in range(0, c, LANE):
                    dg, du, _ = hidden_back(both[:, 2 * k : 2 * (k + LANE)], back[:, k : k + LANE])
                    to = 2 * (j - start + k)
                    dgu[:, to : to + LANE] = dg
                    dgu[:, to + LANE : to + 2 * LANE] = du
            accg[:, :width] += dot(at, dgu[:, :width], 0, 0)
            return 0

        with jax.named_scope(f"chunk_{start}"):
            lax.fori_loop(0, tiles, chunk, 0)
        r = term.shape[2]
        for n in range(SIDE * SIDE):
            term[n // SIDE, n % SIDE] = accg[r * n : r * (n + 1), :width].astype(BF)
    four.advance("A")
    squares = jnp.zeros((1, 1), F32)

    def taken(unit, layer, start):
        unit.advance("E")
        found = jnp.zeros((1, 1), F32)
        for which, half in enumerate(unit.result()):
            wide = half.astype(F32)
            found += jnp.sum(wide * wide, keepdims=True)
            width = half.shape[1]
            if start is None:
                rd[layer, :, which * width : (which + 1) * width] = half
            else:
                for k in range(0, width, LANE):
                    block = (2 * start + which * width + k) // LANE
                    out = (rg, ru)[block % 2]
                    out[layer, :, block // 2 * LANE : (block // 2 + 1) * LANE] = half[:, k : k + LANE]
        return found

    starts = [start for start, _ in chunks]
    three.advance("C")
    two.advance("D")
    squares += taken(gu1, 1, 0) + taken(dd1, 1, None)
    four.advance("C")
    squares += taken(dd0, 0, None) + taken(one, 0, starts[0])
    squares += taken(two, 0, starts[1]) + taken(three, 0, starts[2])
    squares += taken(four, 0, starts[3])
    total[...] = jnp.broadcast_to(sum_everywhere(squares, mine, theirs, send, recv, 16 * n_units), total.shape)
    for unit in units:
        unit.drain()


def back_and_reduced(a, dh, wgu, wd, prod, gu, dd):
    tokens, d = a.shape
    ff = wd.shape[0]
    rows, rows_d = gu.shape[2], dd.shape[2]
    chunks = chunks_of(ff)
    shapes = [gu.shape, dd.shape, dd.shape] + [gu.shape[:3] + (2 * (stop - start),) for start, stop in chunks]
    widest = 2 * max(stop - start for start, stop in chunks)
    scratch = [pltpu.VMEM(shape, BF) for shape in shapes]
    for shape, kind in zip(shapes, kinds_of(len(shapes)), strict=True):
        scratch += kind.scratch(shape[2], shape[3])
    n = 16 * len(shapes) + 6
    return pl.pallas_call(
        functools.partial(back_kernel, chunks),
        in_specs=[pl.BlockSpec(memory_space=pl.ANY)] * 7,
        out_specs=[pl.BlockSpec(memory_space=pltpu.VMEM)] * 4,
        out_shape=[
            jax.ShapeDtypeStruct((2, rows, ff), BF),
            jax.ShapeDtypeStruct((2, rows, ff), BF),
            jax.ShapeDtypeStruct((2, rows_d, d), BF),
            jax.ShapeDtypeStruct((8, LANE), F32),
        ],
        scratch_shapes=scratch
        + [
            pltpu.VMEM((tokens, d), BF),
            pltpu.VMEM((tokens, d), BF),
            pltpu.VMEM((d, 2 * ff), BF),
            pltpu.VMEM((ff, d), BF),
            pltpu.VMEM((2, BACK_TILE, ff), BF),
            pltpu.VMEM((ff, d), F32),
            pltpu.VMEM((d, widest), F32),
            pltpu.VMEM((BACK_TILE, widest), BF),
            pltpu.VMEM((2, 8, LANE), F32),
            pltpu.VMEM((2, SIDE - 1, 8, LANE), F32),
            pltpu.SemaphoreType.DMA((n,)),
            pltpu.SemaphoreType.DMA((n,)),
            pltpu.SemaphoreType.DMA((6,)),
            pltpu.SemaphoreType.DMA((2,)),
        ],
        compiler_params=pltpu.CompilerParams(collective_id=2, has_side_effects=True, vmem_limit_bytes=62 * 2**20),
    )(a, dh, wgu, wd, prod, gu, dd)


def adamw(w, m, v, g):
    m = 0.9 * m + 0.1 * g
    v = 0.95 * v + 0.05 * g * g
    step = m * lax.rsqrt(v + 1e-8) + 0.1 * w
    return (w - 0.02 * step).astype(jnp.bfloat16), m, v


def solution(mesh):
    group = mesh.shape["dp"]

    def step(x, dy, *arrays):
        weights, m, v = (arrays[i : i + 3] for i in (0, 3, 6))
        h0, by1 = x[0], dy[0]
        h1, a0, prod, wgu, wd = forward(h0, *weights)
        by0, gu1, dd1 = layer_back(h1, by1, wgu[1], wd[1])
        *gradients, total = back_and_reduced(a0, by0, wgu[0], wd[0], prod, gu1, dd1)
        count = group * sum(g.size for g in gradients)
        factor = jnp.minimum(1.0, 0.5 * lax.rsqrt(total[0, 0] / count + 1e-30))
        new = [adamw(w.astype(F32), m, v, g.astype(F32) * factor) for w, m, v, g in zip(weights, m, v, gradients, strict=True)]
        return tuple(one[which] for which in range(3) for one in new)

    states, cut = P(("rep", "dp"), None, None), P(None, "dp", None)
    return jax.shard_map(
        step,
        mesh=mesh,
        in_specs=(states, states) + (cut,) * 9,
        out_specs=(P("rep", "dp", None),) * 9,
        check_vma=False,
    )
```

```python
import functools

import jax
import jax.numpy as jnp
from jax import lax
from jax.experimental import pallas as pl
from jax.experimental.pallas import tpu as pltpu
from jax.sharding import PartitionSpec as P

F32, BF = jnp.float32, jnp.bfloat16
MESH = pl.DeviceIdType.MESH
LANE = 128
TILE = 512
FORWARD_TILE = 1024
BACK_TILE = 1024
SIDE = 4
HOPS = (1, -1, 2)


def dot(a, b, ca=1, cb=0):
    return lax.dot_general(a, b, (((ca,), (cb,)), ((), ())), preferred_element_type=F32)


def inverse_rms(wide):
    return lax.rsqrt(jnp.mean(wide * wide, -1, keepdims=True) + 1e-6)


def place():
    me = lax.axis_index("dp")
    return me // SIDE, lax.rem(me, SIDE)


def others():
    return [along(order, by) for order in "yx" for by in HOPS]


def shifted(i, by):
    return lax.rem(i + by + SIDE, SIDE)


def along(order, by, second=False):
    x, y = place()
    if (order == "y") != second:
        return {"dp": x * SIDE + shifted(y, by)}
    return {"dp": shifted(x, by) * SIDE + y}


def ring_places(order):
    x, y = place()
    return (y, x) if order == "y" else (x, y)


def entry_barrier(peers):
    with jax.named_scope("entry"):
        barrier = pltpu.get_barrier_semaphore()
        for peer in peers:
            pl.semaphore_signal(barrier, inc=1, device_id=peer, device_id_type=MESH)
        pl.semaphore_wait(barrier, len(peers))


class Gather:
    def __init__(self, buf, core, cut, rows, send, recv, base, steps):
        self.steps = steps
        self.buf, self.core, self.send, self.recv, self.base = buf, core, send, recv, base
        half = buf.shape[-1] // 2
        self.half, self.rows, self.r = half, rows, buf.shape[-2]
        self.columns = {"y": (0, cut), "x": (cut, half - cut)}

    def at(self, order, first, second, rows=slice(None)):
        off, width = self.columns[order]
        cols = pl.ds(pl.multiple_of(self.core * self.half + off, LANE), width)
        a, b = (second, first) if order == "y" else (first, second)
        return self.buf.at[a, b, rows, cols]

    def hops(self, step):
        straight = (step == "A" and "B" not in self.steps) or (step == "C" and "D" not in self.steps)
        return HOPS if straight else HOPS[:2]

    def copies(self, step):
        out = []
        for which, order in enumerate("yx"):
            i1, i2 = ring_places(order)
            hops = self.hops(step)
            if step == "A":
                refs = [self.at(order, i1, i2)] * len(hops)
            elif step == "B":
                refs = [
                    self.at(order, shifted(i1, -1), i2, pl.ds(0, self.rows)),
                    self.at(order, shifted(i1, 1), i2, pl.ds(self.rows, self.r - self.rows)),
                ]
            elif step == "C":
                refs = [self.at(order, slice(None), i2)] * len(hops)
            else:
                refs = [
                    self.at(order, pl.ds(0, SIDE // 2), shifted(i2, -1)),
                    self.at(order, pl.ds(SIDE // 2, SIDE // 2), shifted(i2, 1)),
                ]
            for side, ref in enumerate(refs):
                before = sum(2 * len(self.hops(one)) for one in self.steps[: self.steps.index(step)])
                number = self.base + before + which * len(hops) + side
                out.append(
                    pltpu.make_async_remote_copy(
                        src_ref=ref,
                        dst_ref=ref,
                        send_sem=self.send.at[number],
                        recv_sem=self.recv.at[number],
                        device_id=along(order, hops[side], step in "CD"),
                        device_id_type=MESH,
                    )
                )
        return out

    def across(self, partner):
        ref = self.buf.at[:, :, :, pl.ds(pl.multiple_of(self.core * self.half, LANE), self.half)]
        number = self.base + 16
        return pltpu.make_async_remote_copy(
            src_ref=ref, dst_ref=ref, send_sem=self.send.at[number], recv_sem=self.recv.at[number], device_id=partner, device_id_type=MESH
        )

    def advance(self, step, partner):
        if step != "A":
            with jax.named_scope(f"wait_{step}{self.base // 17}"):
                for copy in self.copies(self.steps[self.steps.index(step) - 1]):
                    copy.wait_recv()
        if step == "E":
            self.across(partner).start()
        else:
            for copy in self.copies(step):
                copy.start()

    def finish(self, partner):
        with jax.named_scope(f"wait_F{self.base // 17}"):
            self.across(partner).wait_recv()

    def drain(self, partner):
        for step in self.steps[:-1]:
            for copy in self.copies(step):
                copy.wait_send()
        self.across(partner).wait_send()


def pieces_of(ff):
    cuts = [0, 3 * LANE, 7 * LANE, ff]
    return list(zip(cuts[:-1], cuts[1:]))


def forward_kernel(layers, wg_ref, wu_ref, wd_ref, x_hbm, h_hbm, a_hbm, prod_hbm, *refs):
    (ogu, od), refs = (refs[:layers], refs[layers : 2 * layers]), refs[2 * layers :]
    ff = wg_ref.shape[2]
    pieces = pieces_of(ff)
    first, (later, dd, xv, a, prod, wide_d, wd0, send, recv, out_sem, h_sem, p_sem) = refs[: len(pieces)], refs[len(pieces) :]
    tokens, d = xv.shape
    tiles = tokens // FORWARD_TILE
    rep = lax.axis_index("rep")
    core = lax.rem(rep, 2)
    partner = {"rep": rep + 1 - 2 * core}
    x, y = place()
    x_load = pltpu.make_async_copy(x_hbm, xv, out_sem.at[0])
    x_load.start()

    def placed(buf, layer, start, stop):
        for k in range(start, stop, LANE):
            at = 2 * (k - start)
            buf[x, y, :, at : at + LANE] = wg_ref[layer, :, k : k + LANE]
            buf[x, y, :, at + LANE : at + 2 * LANE] = wu_ref[layer, :, k : k + LANE]

    bufs = list(first) + [dd.at[0]]
    for buf, (start, stop) in zip(first, pieces, strict=True):
        placed(buf, 0, start, stop)
    for layer in range(1, layers):
        placed(later.at[layer - 1], layer, 0, ff)
        bufs += [later.at[layer - 1], dd.at[layer]]
    for layer in range(layers):
        dd[layer, x, y] = wd_ref[layer]
    entry_barrier(others() + [partner])

    def unit_of(n, buf):
        steps = "ACE" if n == 0 else "ACDE" if n <= len(pieces) else "ABCDE"
        quarter = (buf.shape[-1] // 4 + LANE - 1) // LANE * LANE
        return Gather(buf, core, quarter, 16 if buf.shape[2] % 32 == 0 else 48, send, recv, 17 * n, steps)

    units = [unit_of(n, buf) for n, buf in enumerate(bufs)]
    gus, down, rest = units[: len(pieces)], units[len(pieces)], units[len(pieces) + 1 :]
    one, two, three = gus

    def go(step, *those):
        for unit in those:
            unit.advance(step, partner)

    go("A", *gus, down)
    x_load.wait()

    def norm(t, _):
        rows = pl.ds(pl.multiple_of(t * FORWARD_TILE, FORWARD_TILE), FORWARD_TILE)
        wide = xv[rows].astype(F32)
        a[rows] = (wide * inverse_rms(wide)).astype(BF)
        return 0

    with jax.named_scope("norm"):
        lax.fori_loop(0, tiles, norm, 0)
    go("C", one, two, three, down)
    go("E", one)
    slots = [
        {0: [("D", [two])], 2: [("D", [three])], 4: [("D", [down]), ("A", rest)], 6: [("E", [two])]},
        {0: [("E", [three]), ("B", rest)], 2: [("E", [down])], 4: [("C", rest)]},
        {},
    ]
    for unit, buf, (start, stop), slot in zip(gus, first, pieces, slots, strict=True):
        unit.finish(partner)

        def products(t, _):
            for when, actions in slot.items():

                @pl.when(t == when * tiles // 8)
                def _():
                    for step, those in actions:
                        go(step, *those)

            rows = pl.ds(pl.multiple_of(t * FORWARD_TILE, FORWARD_TILE), FORWARD_TILE)
            at = a[rows]
            for j in range(start, stop, 2 * LANE):
                c = min(2 * LANE, stop - j)
                w = buf[:, :, :, 2 * (j - start) : 2 * (j - start + c)].reshape(d, 2 * c)
                both = dot(at, w)
                for k in range(0, c, LANE):
                    g, u = both[:, 2 * k : 2 * k + LANE], both[:, 2 * k + LANE : 2 * k + 2 * LANE]
                    prod[rows, j + k : j + k + LANE] = (g * jax.nn.sigmoid(g) * u).astype(BF)
            return 0

        with jax.named_scope(f"products_{start}"):
            lax.fori_loop(0, tiles, products, 0)

    def gu_out(n):
        start, stop = pieces[n]
        return pltpu.make_async_copy(first[n], ogu[0].at[:, :, :, 2 * start : 2 * stop], out_sem.at[n])

    a_out = pltpu.make_async_copy(a, a_hbm, h_sem.at[tiles])
    a_out.start()
    outs = [gu_out(n) for n in range(len(pieces))] + [pltpu.make_async_copy(dd.at[0], od[0], out_sem.at[len(pieces)])]
    for layer in range(1, layers):
        n = len(outs)
        outs.append(pltpu.make_async_copy(later.at[layer - 1], ogu[layer], out_sem.at[n]))
        outs.append(pltpu.make_async_copy(dd.at[layer], od[layer], out_sem.at[n + 1]))
    down.finish(partner)
    for copy in outs[: len(pieces) + 1]:
        copy.start()
    r = dd.shape[3]
    for n in range(SIDE * SIDE):
        wide_d[r * n : r * (n + 1)] = dd[0, n // SIDE, n % SIDE].astype(F32)
    wd0[...] = wide_d[...].astype(BF)

    def tile_outs(t):
        rows = pl.ds(pl.multiple_of(t * FORWARD_TILE, FORWARD_TILE), FORWARD_TILE)
        return [pltpu.make_async_copy(xv.at[rows], h_hbm.at[rows], h_sem.at[t]), pltpu.make_async_copy(prod.at[rows], prod_hbm.at[rows], p_sem.at[t])]

    def close(t, _):
        for when, step in ((0, "D"), (tiles // 2, "E")):

            @pl.when(t == when)
            def _():
                go(step, *rest)

        rows = pl.ds(pl.multiple_of(t * FORWARD_TILE, FORWARD_TILE), FORWARD_TILE)
        xv[rows] = xv[rows] + dot(prod[rows], wd0[...]).astype(BF)
        for copy in tile_outs(t):
            copy.start()
        return 0

    with jax.named_scope("close"):
        lax.fori_loop(0, tiles, close, 0)
    for unit in rest:
        unit.finish(partner)
    for copy in outs[len(pieces) + 1 :]:
        copy.start()
    for unit in units:
        unit.drain(partner)

    def closed(t, _):
        for copy in tile_outs(t):
            copy.wait()
        return 0

    with jax.named_scope("out_wait"):
        lax.fori_loop(0, tiles, closed, 0)
        for copy in outs + [a_out]:
            copy.wait()


def forward(x, wg, wu, wd):
    tokens, d = x.shape
    layers, rows, ff = wg.shape
    rows_d = wd.shape[1]
    pieces = pieces_of(ff)
    n = 17 * (len(pieces) + 2 * layers - 1)
    anywhere = pl.BlockSpec(memory_space=pl.ANY)
    h, a, prod, *full = pl.pallas_call(
        functools.partial(forward_kernel, layers),
        in_specs=[pl.BlockSpec(memory_space=pltpu.VMEM)] * 3 + [anywhere],
        out_specs=[anywhere] * (3 + 2 * layers),
        out_shape=[jax.ShapeDtypeStruct((tokens, d), BF)] * 2
        + [jax.ShapeDtypeStruct((tokens, ff), BF)]
        + [jax.ShapeDtypeStruct((SIDE, SIDE, rows, 2 * ff), BF)] * layers
        + [jax.ShapeDtypeStruct((SIDE, SIDE, rows_d, d), BF)] * layers,
        scratch_shapes=[pltpu.VMEM((SIDE, SIDE, rows, 2 * (stop - start)), BF) for start, stop in pieces]
        + [
            pltpu.VMEM((layers - 1, SIDE, SIDE, rows, 2 * ff), BF),
            pltpu.VMEM((layers, SIDE, SIDE, rows_d, d), BF),
            pltpu.VMEM((tokens, d), BF),
            pltpu.VMEM((tokens, d), BF),
            pltpu.VMEM((tokens, ff), BF),
            pltpu.VMEM((ff, d), F32),
            pltpu.VMEM((ff, d), BF),
            pltpu.SemaphoreType.DMA((n,)),
            pltpu.SemaphoreType.DMA((n,)),
            pltpu.SemaphoreType.DMA((len(pieces) + 2 * layers - 1,)),
            pltpu.SemaphoreType.DMA((tokens // FORWARD_TILE + 1,)),
            pltpu.SemaphoreType.DMA((tokens // FORWARD_TILE,)),
        ],
        compiler_params=pltpu.CompilerParams(collective_id=1, has_side_effects=True, vmem_limit_bytes=60 * 2**20),
    )(wg, wu, wd, x)
    return h, a, prod, [one.reshape(d, 2 * ff) for one in full[:layers]], [one.reshape(ff, d) for one in full[layers:]]


def hidden_back(both, by):
    g, u, b = both[:, :LANE], both[:, LANE:], by.astype(BF).astype(F32)
    s = jax.nn.sigmoid(g)
    silu = g * s
    return (b * u * (s + silu * (1 - s))).astype(BF), (b * silu).astype(BF), (silu * u).astype(BF)


def layer_kernel(h_ref, dy_ref, wgu_ref, wd_ref, dh_ref, dwgu_ref, dwd_ref, accgu, accd, dgu, prod):
    step, steps = pl.program_id(0), pl.num_programs(0)
    ff = wd_ref.shape[0]

    @pl.when(step == 0)
    def _():
        accgu[...] = jnp.zeros_like(accgu)
        accd[...] = jnp.zeros_like(accd)

    wide = h_ref[...].astype(F32)
    scale = inverse_rms(wide)
    a = (wide * scale).astype(BF)
    dy = dy_ref[...]
    for j in range(0, ff, 2 * LANE):
        c = min(2 * LANE, ff - j)
        both = dot(a, wgu_ref[:, 2 * j : 2 * (j + c)])
        by = dot(dy, wd_ref[j : j + c, :], 1, 1)
        for k in range(0, c, LANE):
            at = j + k
            dg, du, product = hidden_back(both[:, 2 * k : 2 * (k + LANE)], by[:, k : k + LANE])
            prod[:, at : at + LANE] = product
            dgu[:, 2 * at : 2 * at + LANE] = dg
            dgu[:, 2 * at + LANE : 2 * at + 2 * LANE] = du
    da = dot(dgu[...], wgu_ref[...], 1, 1)
    back = scale * (da - wide * (scale * scale * jnp.mean(da * wide, -1, keepdims=True)))
    dh_ref[...] = dy + back.astype(BF)
    accgu[...] += dot(a, dgu[...], 0, 0)
    accd[...] += dot(prod[...], dy, 0, 0)

    @pl.when(step == steps - 1)
    def _():
        r, q = dwgu_ref.shape[2], dwd_ref.shape[2]
        for d in range(SIDE * SIDE):
            dwgu_ref[d // SIDE, d % SIDE] = accgu[r * d : r * (d + 1)].astype(BF)
            dwd_ref[d // SIDE, d % SIDE] = accd[q * d : q * (d + 1)].astype(BF)


def layer_back(h, dy, wgu, wd):
    tokens, d = h.shape
    ff = wd.shape[0]
    n = SIDE * SIDE
    tile = pl.BlockSpec((TILE, d), lambda i: (i, 0))
    whole = lambda shape: pl.BlockSpec(shape, lambda i: (0,) * len(shape))
    gu, dd = (SIDE, SIDE, d // n, 2 * ff), (SIDE, SIDE, ff // n, d)
    return pl.pallas_call(
        layer_kernel,
        grid=(tokens // TILE,),
        in_specs=[tile, tile, whole(wgu.shape), whole(wd.shape)],
        out_specs=[tile, whole(gu), whole(dd)],
        out_shape=[jax.ShapeDtypeStruct((tokens, d), BF), jax.ShapeDtypeStruct(gu, BF), jax.ShapeDtypeStruct(dd, BF)],
        scratch_shapes=[
            pltpu.VMEM((d, 2 * ff), F32),
            pltpu.VMEM((ff, d), F32),
            pltpu.VMEM((TILE, 2 * ff), BF),
            pltpu.VMEM((TILE, ff), BF),
        ],
        compiler_params=pltpu.CompilerParams(vmem_limit_bytes=60 * 2**20),
    )(h, dy, wgu, wd)


class Scatter:
    def __init__(self, terms, bufs, send, recv, base):
        self.terms, self.send, self.recv, self.base = terms, send, recv, base
        self.a, self.b, self.sums, self.out, self.c, self.d = bufs
        self.half = terms.shape[-1] // 2
        r = terms.shape[2]
        if r % 32 == 0:
            self.parts = [(pl.ds(0, r // 2), slice(None)), (pl.ds(r // 2, r // 2), slice(None))]
        else:
            q = self.half // 2
            self.parts = [(slice(None), pl.ds(0, q)), (slice(None), pl.ds(q, q))]

    @staticmethod
    def scratch(rows, columns):
        half = columns // 2
        return [
            pltpu.VMEM((2, 2, SIDE // 2, rows, half), BF),
            pltpu.VMEM((2, 2, SIDE, rows, half), BF),
            pltpu.VMEM((2, SIDE, rows, half), F32),
            pltpu.VMEM((2, SIDE, rows, half), BF),
            pltpu.VMEM((2, rows, half), BF),
            pltpu.VMEM((2, 2, rows, half), BF),
        ]

    def index(self, which, first, second):
        cols = pl.ds(which * self.half, self.half)
        return (second, first, slice(None), cols) if which == 0 else (first, second, slice(None), cols)

    def copies(self, step):
        out = []
        for which, order in enumerate("yx"):
            i1, i2 = ring_places(order)
            for side in range(2):
                by = 1 - 2 * side
                if step == "A":
                    src = self.terms.at[self.index(which, shifted(i1, 2), pl.ds(side * (SIDE // 2), SIDE // 2))]
                    dst = self.a.at[which, side]
                elif step == "B":
                    src = self.terms.at[self.index(which, shifted(i1, by), slice(None))]
                    dst = self.b.at[which, side]
                elif step == "C":
                    rows, cols = self.parts[side]
                    src = self.out.at[which, shifted(i2, 2), rows, cols]
                    dst = self.c.at[which, rows, cols]
                else:
                    src = self.out.at[which, shifted(i2, by)]
                    dst = self.d.at[which, side]
                number = self.base + "ABCD".index(step) * 4 + which * 2 + side
                out.append(
                    pltpu.make_async_remote_copy(
                        src_ref=src,
                        dst_ref=dst,
                        send_sem=self.send.at[number],
                        recv_sem=self.recv.at[number],
                        device_id=along(order, by, step in "CD"),
                        device_id_type=MESH,
                    )
                )
        return out

    def advance(self, step):
        if step != "A":
            with jax.named_scope(f"wait_{step}{self.base // 16}"):
                for copy in self.copies("ABCD"["ABCDE".index(step) - 1]):
                    copy.wait_recv()
        for which, order in enumerate("yx"):
            i1, i2 = ring_places(order)
            if step == "B":
                for side in range(2):
                    for k in range(SIDE // 2):
                        at = self.index(which, shifted(i1, 1 - 2 * side), side * (SIDE // 2) + k)
                        self.terms[at] = (self.terms[at].astype(F32) + self.a[which, side, k].astype(F32)).astype(BF)
            elif step == "C":

                def own(k, _):
                    mine = self.terms[self.index(which, i1, k)].astype(F32)
                    self.sums[which, k] = mine + self.b[which, 0, k].astype(F32) + self.b[which, 1, k].astype(F32)
                    return 0

                lax.fori_loop(0, SIDE, own, 0)
                far = shifted(i2, 2)
                self.out[which, far] = self.sums[which, far].astype(BF)
            elif step == "D":
                for side in range(2):
                    near = shifted(i2, 1 - 2 * side)
                    for part in range(2):
                        at = self.parts[part]
                        value = self.sums[(which, near) + at]
                        if part == side:
                            value = value + self.c[(which,) + at].astype(F32)
                        self.out[(which, near) + at] = value.astype(BF)
        if step != "E":
            for copy in self.copies(step):
                copy.start()

    def result(self):
        halves = []
        for which, order in enumerate("yx"):
            _, i2 = ring_places(order)
            total = self.sums[which, i2] + self.d[which, 0].astype(F32) + self.d[which, 1].astype(F32)
            halves.append(total.astype(BF))
        return halves

    def drain(self):
        for step in "ABCD":
            for copy in self.copies(step):
                copy.wait_send()


class DirectScatter(Scatter):
    def __init__(self, terms, bufs, send, recv, base):
        self.terms, self.send, self.recv, self.base = terms, send, recv, base
        self.b, self.sums, self.out, self.d = bufs
        self.half = terms.shape[-1] // 2

    @staticmethod
    def scratch(rows, columns):
        half = columns // 2
        return [
            pltpu.VMEM((2, len(HOPS), SIDE, rows, half), BF),
            pltpu.VMEM((2, SIDE, rows, half), F32),
            pltpu.VMEM((2, SIDE, rows, half), BF),
            pltpu.VMEM((2, len(HOPS), rows, half), BF),
        ]

    def copies(self, step):
        out = []
        for which, order in enumerate("yx"):
            i1, i2 = ring_places(order)
            for k, by in enumerate(HOPS):
                if step == "A":
                    src, dst = self.terms.at[self.index(which, shifted(i1, by), slice(None))], self.b.at[which, k]
                else:
                    src, dst = self.out.at[which, shifted(i2, by)], self.d.at[which, k]
                number = self.base + (step == "C") * 6 + which * 3 + k
                out.append(
                    pltpu.make_async_remote_copy(
                        src_ref=src,
                        dst_ref=dst,
                        send_sem=self.send.at[number],
                        recv_sem=self.recv.at[number],
                        device_id=along(order, by, step == "C"),
                        device_id_type=MESH,
                    )
                )
        return out

    def advance(self, step):
        if step != "A":
            with jax.named_scope(f"wait_{step}{self.base // 16}"):
                for copy in self.copies("A" if step == "C" else "C"):
                    copy.wait_recv()
        if step == "C":
            for which, order in enumerate("yx"):
                i1, _ = ring_places(order)
                for k in range(SIDE):
                    total = self.terms[self.index(which, i1, k)].astype(F32)
                    for n in range(len(HOPS)):
                        total += self.b[which, n, k].astype(F32)
                    self.sums[which, k] = total
                    self.out[which, k] = total.astype(BF)
        if step != "E":
            for copy in self.copies(step):
                copy.start()

    def result(self):
        halves = []
        for which, order in enumerate("yx"):
            _, i2 = ring_places(order)
            total = self.sums[which, i2]
            for n in range(len(HOPS)):
                total += self.d[which, n].astype(F32)
            halves.append(total.astype(BF))
        return halves

    def drain(self):
        for step in "AC":
            for copy in self.copies(step):
                copy.wait_send()


def sum_everywhere(value, mine, theirs, send, recv, base):
    for which, order in enumerate("yx"):
        mine[which] = jnp.broadcast_to(value, mine.shape[1:])
        copies = [
            pltpu.make_async_remote_copy(
                src_ref=mine.at[which],
                dst_ref=theirs.at[which, by - 1],
                send_sem=send.at[base + which * 3 + by - 1],
                recv_sem=recv.at[base + which * 3 + by - 1],
                device_id=along(order, by),
                device_id_type=MESH,
            )
            for by in range(1, SIDE)
        ]
        with jax.named_scope(f"squares_{order}"):
            for copy in copies:
                copy.start()
            for copy in copies:
                copy.wait()
        value = value + theirs[which, 0][:1, :1] + theirs[which, 1][:1, :1] + theirs[which, 2][:1, :1]
    return value


def chunks_of(ff):
    cuts = [0, 4 * LANE, 8 * LANE, ff - LANE, ff]
    return list(zip(cuts[:-1], cuts[1:]))


def kinds_of(units):
    return [Scatter] * (units - 2) + [DirectScatter] * 2


def back_kernel(chunks, a_hbm, dh_hbm, wgu_hbm, wd_hbm, prod_hbm, gu_hbm, dd_hbm, rg, ru, rd, total, *refs):
    n_units = 3 + len(chunks)
    terms, refs = refs[:n_units], refs[n_units:]
    units = []
    for n, kind in enumerate(kinds_of(n_units)):
        count = len(kind.scratch(1, 2))
        units.append((kind, terms[n], refs[:count], 16 * n))
        refs = refs[count:]
    a, dh, wgu, wd, pbuf, accd, accg, dgu, mine, theirs, send, recv, load, p_sem = refs
    tokens, d = a.shape
    tiles = tokens // BACK_TILE
    units = [kind(term, bufs, send, recv, base) for kind, term, bufs, base in units]
    gu1, dd1, dd0, *parts = units
    pairs = [(gu_hbm, terms[0]), (dd_hbm, terms[1]), (dh_hbm, dh), (a_hbm, a), (wgu_hbm, wgu), (wd_hbm, wd)]
    loads = [pltpu.make_async_copy(source, to, load.at[n]) for n, (source, to) in enumerate(pairs)]
    rows_of = lambda t: pl.ds(pl.multiple_of(t * BACK_TILE, BACK_TILE), BACK_TILE)
    prod_load = lambda t: pltpu.make_async_copy(prod_hbm.at[rows_of(t)], pbuf.at[lax.rem(t, 2)], p_sem.at[lax.rem(t, 2)])
    for copy in loads[:3]:
        copy.start()
    prod_load(0).start()
    entry_barrier(others())
    for copy, unit in zip(loads[:2], units[:2], strict=True):
        copy.wait()
        unit.advance("A")
    loads[2].wait()
    accd[...] = jnp.zeros_like(accd)

    def down(t, _):
        @pl.when(t + 1 < tiles)
        def _():
            prod_load(t + 1).start()

        @pl.when(t == 0)
        def _():
            for copy in loads[3:]:
                copy.start()

        rows = rows_of(t)
        prod_load(t).wait()
        accd[...] += dot(pbuf[lax.rem(t, 2)], dh[rows], 0, 0)
        return 0

    with jax.named_scope("down"):
        lax.fori_loop(0, tiles, down, 0)
    q = terms[2].shape[2]
    for n in range(SIDE * SIDE):
        terms[2][n // SIDE, n % SIDE] = accd[q * n : q * (n + 1)].astype(BF)
    gu1.advance("B")
    for copy in loads[3:]:
        copy.wait()
    one, two, three, four = parts
    slots = [
        {4: [(dd1, "B"), (dd0, "A")]},
        {0: [(gu1, "C"), (one, "A")], 2: [(dd1, "C"), (dd0, "B")], 4: [(gu1, "D"), (one, "B")], 6: [(dd1, "D"), (dd0, "C")]},
        {0: [(two, "A")], 2: [(one, "C"), (dd0, "D")], 4: [(two, "B")], 6: [(one, "D")]},
        {0: [(three, "A")], 4: [(two, "C")]},
    ]
    for (start, stop), term, slot in zip(chunks, terms[3:], slots, strict=True):
        width = 2 * (stop - start)
        tile = BACK_TILE if stop < chunks[-1][1] else 2 * BACK_TILE
        tiles = tokens // tile
        accg[:, :width] = jnp.zeros((d, width), F32)

        def chunk(t, _):
            for when, actions in slot.items():

                @pl.when(t == when * tiles // 8)
                def _():
                    for unit, step in actions:
                        unit.advance(step)

            rows = pl.ds(pl.multiple_of(t * tile, tile), tile)
            at, by = a[rows], dh[rows]
            to_rows = pl.ds(0, tile)
            for j in range(start, stop, 2 * LANE):
                c = min(2 * LANE, stop - j)
                both = dot(at, wgu[:, 2 * j : 2 * (j + c)])
                back = dot(by, wd[j : j + c, :], 1, 1)
                for k in range(0, c, LANE):
                    dg, du, _ = hidden_back(both[:, 2 * k : 2 * (k + LANE)], back[:, k : k + LANE])
                    to = 2 * (j - start + k)
                    dgu[to_rows, to : to + LANE] = dg
                    dgu[to_rows, to + LANE : to + 2 * LANE] = du
            accg[:, :width] += dot(at, dgu[to_rows, :width], 0, 0)
            return 0

        with jax.named_scope(f"chunk_{start}"):
            lax.fori_loop(0, tiles, chunk, 0)
        r = term.shape[2]
        for n in range(SIDE * SIDE):
            term[n // SIDE, n % SIDE] = accg[r * n : r * (n + 1), :width].astype(BF)
    four.advance("A")
    squares = jnp.zeros((1, 1), F32)

    def taken(unit, layer, start):
        unit.advance("E")
        found = jnp.zeros((1, 1), F32)
        for which, half in enumerate(unit.result()):
            wide = half.astype(F32)
            found += jnp.sum(wide * wide, keepdims=True)
            width = half.shape[1]
            if start is None:
                rd[layer, :, which * width : (which + 1) * width] = half
            else:
                for k in range(0, width, LANE):
                    block = (2 * start + which * width + k) // LANE
                    out = (rg, ru)[block % 2]
                    out[layer, :, block // 2 * LANE : (block // 2 + 1) * LANE] = half[:, k : k + LANE]
        return found

    starts = [start for start, _ in chunks]
    three.advance("C")
    two.advance("D")
    squares += taken(gu1, 1, 0) + taken(dd1, 1, None)
    four.advance("C")
    squares += taken(dd0, 0, None) + taken(one, 0, starts[0])
    squares += taken(two, 0, starts[1]) + taken(three, 0, starts[2])
    squares += taken(four, 0, starts[3])
    total[...] = jnp.broadcast_to(sum_everywhere(squares, mine, theirs, send, recv, 16 * n_units), total.shape)
    for unit in units:
        unit.drain()


def back_and_reduced(a, dh, wgu, wd, prod, gu, dd):
    tokens, d = a.shape
    ff = wd.shape[0]
    rows, rows_d = gu.shape[2], dd.shape[2]
    chunks = chunks_of(ff)
    shapes = [gu.shape, dd.shape, dd.shape] + [gu.shape[:3] + (2 * (stop - start),) for start, stop in chunks]
    widest = 2 * max(stop - start for start, stop in chunks)
    scratch = [pltpu.VMEM(shape, BF) for shape in shapes]
    for shape, kind in zip(shapes, kinds_of(len(shapes)), strict=True):
        scratch += kind.scratch(shape[2], shape[3])
    n = 16 * len(shapes) + 6
    return pl.pallas_call(
        functools.partial(back_kernel, chunks),
        in_specs=[pl.BlockSpec(memory_space=pl.ANY)] * 7,
        out_specs=[pl.BlockSpec(memory_space=pltpu.VMEM)] * 4,
        out_shape=[
            jax.ShapeDtypeStruct((2, rows, ff), BF),
            jax.ShapeDtypeStruct((2, rows, ff), BF),
            jax.ShapeDtypeStruct((2, rows_d, d), BF),
            jax.ShapeDtypeStruct((8, LANE), F32),
        ],
        scratch_shapes=scratch
        + [
            pltpu.VMEM((tokens, d), BF),
            pltpu.VMEM((tokens, d), BF),
            pltpu.VMEM((d, 2 * ff), BF),
            pltpu.VMEM((ff, d), BF),
            pltpu.VMEM((2, BACK_TILE, ff), BF),
            pltpu.VMEM((ff, d), F32),
            pltpu.VMEM((d, widest), F32),
            pltpu.VMEM((2 * BACK_TILE, widest), BF),
            pltpu.VMEM((2, 8, LANE), F32),
            pltpu.VMEM((2, SIDE - 1, 8, LANE), F32),
            pltpu.SemaphoreType.DMA((n,)),
            pltpu.SemaphoreType.DMA((n,)),
            pltpu.SemaphoreType.DMA((6,)),
            pltpu.SemaphoreType.DMA((2,)),
        ],
        compiler_params=pltpu.CompilerParams(collective_id=2, has_side_effects=True, vmem_limit_bytes=62 * 2**20),
    )(a, dh, wgu, wd, prod, gu, dd)


def adamw(w, m, v, g):
    m = 0.9 * m + 0.1 * g
    v = 0.95 * v + 0.05 * g * g
    step = m * lax.rsqrt(v + 1e-8) + 0.1 * w
    return (w - 0.02 * step).astype(jnp.bfloat16), m, v


def update_kernel(count, total_ref, *refs):
    inputs, outputs = refs[:12], refs[12:]
    factor = jnp.minimum(1.0, 0.5 * lax.rsqrt(total_ref[:1, :1] / count + 1e-30))
    for i in range(3):
        w, m, v, g = inputs[i::3]
        for layer in range(w.shape[0]):
            new = adamw(w[layer].astype(F32), m[layer], v[layer], g[layer].astype(F32) * factor)
            for to, value in zip(outputs[i::3], new, strict=True):
                to[layer] = value


def updated(count, total, weights, m, v, gradients):
    inputs = [*weights, *m, *v, *gradients]
    return pl.pallas_call(
        functools.partial(update_kernel, count),
        in_specs=[pl.BlockSpec(memory_space=pltpu.VMEM)] * 13,
        out_specs=[pl.BlockSpec(memory_space=pltpu.VMEM)] * 9,
        out_shape=[jax.ShapeDtypeStruct(one.shape, one.dtype) for one in inputs[:9]],
        compiler_params=pltpu.CompilerParams(vmem_limit_bytes=62 * 2**20),
    )(total, *inputs)


def solution(mesh):
    group = mesh.shape["dp"]

    def step(x, dy, *arrays):
        weights, m, v = (arrays[i : i + 3] for i in (0, 3, 6))
        h0, by1 = x[0], dy[0]
        h1, a0, prod, wgu, wd = forward(h0, *weights)
        by0, gu1, dd1 = layer_back(h1, by1, wgu[1], wd[1])
        *gradients, total = back_and_reduced(a0, by0, wgu[0], wd[0], prod, gu1, dd1)
        count = group * sum(g.size for g in gradients)
        return tuple(updated(count, total, weights, m, v, gradients))

    states, cut = P(("rep", "dp"), None, None), P(None, "dp", None)
    return jax.shard_map(
        step,
        mesh=mesh,
        in_specs=(states, states) + (cut,) * 9,
        out_specs=(P("rep", "dp", None),) * 9,
        check_vma=False,
    )
```

```python
import functools

import jax
import jax.numpy as jnp
from jax import lax
from jax.experimental import pallas as pl
from jax.experimental.pallas import tpu as pltpu
from jax.sharding import PartitionSpec as P

F32, BF = jnp.float32, jnp.bfloat16
MESH = pl.DeviceIdType.MESH
LANE = 128
TILE = 512
FORWARD_TILE = 1024
BACK_TILE = 1024
SIDE = 4
HOPS = (1, -1, 2)


def dot(a, b, ca=1, cb=0):
    return lax.dot_general(a, b, (((ca,), (cb,)), ((), ())), preferred_element_type=F32)


def inverse_rms(wide):
    return lax.rsqrt(jnp.mean(wide * wide, -1, keepdims=True) + 1e-6)


def place():
    me = lax.axis_index("dp")
    return me // SIDE, lax.rem(me, SIDE)


def others():
    return [along(order, by) for order in "yx" for by in HOPS]


def shifted(i, by):
    return lax.rem(i + by + SIDE, SIDE)


def along(order, by, second=False):
    x, y = place()
    if (order == "y") != second:
        return {"dp": x * SIDE + shifted(y, by)}
    return {"dp": shifted(x, by) * SIDE + y}


def ring_places(order):
    x, y = place()
    return (y, x) if order == "y" else (x, y)


def entry_barrier(peers):
    with jax.named_scope("entry"):
        barrier = pltpu.get_barrier_semaphore()
        for peer in peers:
            pl.semaphore_signal(barrier, inc=1, device_id=peer, device_id_type=MESH)
        pl.semaphore_wait(barrier, len(peers))


class Gather:
    def __init__(self, buf, core, cut, rows, send, recv, base, steps):
        self.steps = steps
        self.buf, self.core, self.send, self.recv, self.base = buf, core, send, recv, base
        half = buf.shape[-1] // 2
        self.half, self.rows, self.r = half, rows, buf.shape[-2]
        self.columns = {"y": (0, cut), "x": (cut, half - cut)}

    def at(self, order, first, second, rows=slice(None)):
        off, width = self.columns[order]
        cols = pl.ds(pl.multiple_of(self.core * self.half + off, LANE), width)
        a, b = (second, first) if order == "y" else (first, second)
        return self.buf.at[a, b, rows, cols]

    def hops(self, step):
        straight = (step == "A" and "B" not in self.steps) or (step == "C" and "D" not in self.steps)
        return HOPS if straight else HOPS[:2]

    def copies(self, step):
        out = []
        for which, order in enumerate("yx"):
            i1, i2 = ring_places(order)
            hops = self.hops(step)
            if step == "A":
                refs = [self.at(order, i1, i2)] * len(hops)
            elif step == "B":
                refs = [
                    self.at(order, shifted(i1, -1), i2, pl.ds(0, self.rows)),
                    self.at(order, shifted(i1, 1), i2, pl.ds(self.rows, self.r - self.rows)),
                ]
            elif step == "C":
                refs = [self.at(order, slice(None), i2)] * len(hops)
            else:
                refs = [
                    self.at(order, pl.ds(0, SIDE // 2), shifted(i2, -1)),
                    self.at(order, pl.ds(SIDE // 2, SIDE // 2), shifted(i2, 1)),
                ]
            for side, ref in enumerate(refs):
                before = sum(2 * len(self.hops(one)) for one in self.steps[: self.steps.index(step)])
                number = self.base + before + which * len(hops) + side
                out.append(
                    pltpu.make_async_remote_copy(
                        src_ref=ref,
                        dst_ref=ref,
                        send_sem=self.send.at[number],
                        recv_sem=self.recv.at[number],
                        device_id=along(order, hops[side], step in "CD"),
                        device_id_type=MESH,
                    )
                )
        return out

    def across(self, partner):
        ref = self.buf.at[:, :, :, pl.ds(pl.multiple_of(self.core * self.half, LANE), self.half)]
        number = self.base + 16
        return pltpu.make_async_remote_copy(
            src_ref=ref, dst_ref=ref, send_sem=self.send.at[number], recv_sem=self.recv.at[number], device_id=partner, device_id_type=MESH
        )

    def advance(self, step, partner):
        if step != "A":
            with jax.named_scope(f"wait_{step}{self.base // 17}"):
                for copy in self.copies(self.steps[self.steps.index(step) - 1]):
                    copy.wait_recv()
        if step == "E":
            self.across(partner).start()
        else:
            for copy in self.copies(step):
                copy.start()

    def finish(self, partner):
        with jax.named_scope(f"wait_F{self.base // 17}"):
            self.across(partner).wait_recv()

    def drain(self, partner):
        for step in self.steps[:-1]:
            for copy in self.copies(step):
                copy.wait_send()
        self.across(partner).wait_send()


def pieces_of(ff):
    cuts = [0, 3 * LANE, 7 * LANE, ff]
    return list(zip(cuts[:-1], cuts[1:]))


def forward_kernel(layers, wg_ref, wu_ref, wd_ref, x_hbm, h_hbm, a_hbm, prod_hbm, *refs):
    (ogu, od), refs = (refs[:layers], refs[layers : 2 * layers]), refs[2 * layers :]
    ff = wg_ref.shape[2]
    pieces = pieces_of(ff)
    first, (later, dd, xv, a, prod, wide_d, wd0, send, recv, out_sem, h_sem, p_sem) = refs[: len(pieces)], refs[len(pieces) :]
    tokens, d = xv.shape
    tiles = tokens // FORWARD_TILE
    rep = lax.axis_index("rep")
    core = lax.rem(rep, 2)
    partner = {"rep": rep + 1 - 2 * core}
    x, y = place()
    x_load = pltpu.make_async_copy(x_hbm, xv, out_sem.at[0])
    x_load.start()

    def placed(buf, layer, start, stop):
        for k in range(start, stop, LANE):
            at = 2 * (k - start)
            buf[x, y, :, at : at + LANE] = wg_ref[layer, :, k : k + LANE]
            buf[x, y, :, at + LANE : at + 2 * LANE] = wu_ref[layer, :, k : k + LANE]

    bufs = list(first) + [dd.at[0]]
    for buf, (start, stop) in zip(first, pieces, strict=True):
        placed(buf, 0, start, stop)
    for layer in range(1, layers):
        placed(later.at[layer - 1], layer, 0, ff)
        bufs += [later.at[layer - 1], dd.at[layer]]
    for layer in range(layers):
        dd[layer, x, y] = wd_ref[layer]
    entry_barrier(others() + [partner])

    def unit_of(n, buf):
        steps = "ACE" if n == 0 else "ACDE" if n <= len(pieces) else "ABCDE"
        quarter = (buf.shape[-1] // 4 + LANE - 1) // LANE * LANE
        return Gather(buf, core, quarter, 16 if buf.shape[2] % 32 == 0 else 48, send, recv, 17 * n, steps)

    units = [unit_of(n, buf) for n, buf in enumerate(bufs)]
    gus, down, rest = units[: len(pieces)], units[len(pieces)], units[len(pieces) + 1 :]
    one, two, three = gus

    def go(step, *those):
        for unit in those:
            unit.advance(step, partner)

    go("A", *gus, down)
    x_load.wait()

    def norm(t, _):
        rows = pl.ds(pl.multiple_of(t * FORWARD_TILE, FORWARD_TILE), FORWARD_TILE)
        wide = xv[rows].astype(F32)
        a[rows] = (wide * inverse_rms(wide)).astype(BF)
        return 0

    with jax.named_scope("norm"):
        lax.fori_loop(0, tiles, norm, 0)
    go("C", one, two, three, down)
    go("E", one)
    slots = [
        {0: [("D", [two])], 2: [("D", [three])], 4: [("D", [down]), ("A", rest)], 6: [("E", [two])]},
        {0: [("E", [three]), ("B", rest)], 2: [("E", [down])], 4: [("C", rest)]},
        {},
    ]
    for unit, buf, (start, stop), slot in zip(gus, first, pieces, slots, strict=True):
        unit.finish(partner)

        def products(t, _):
            for when, actions in slot.items():

                @pl.when(t == when * tiles // 8)
                def _():
                    for step, those in actions:
                        go(step, *those)

            rows = pl.ds(pl.multiple_of(t * FORWARD_TILE, FORWARD_TILE), FORWARD_TILE)
            at = a[rows]
            for j in range(start, stop, 2 * LANE):
                c = min(2 * LANE, stop - j)
                w = buf[:, :, :, 2 * (j - start) : 2 * (j - start + c)].reshape(d, 2 * c)
                both = dot(at, w)
                for k in range(0, c, LANE):
                    g, u = both[:, 2 * k : 2 * k + LANE], both[:, 2 * k + LANE : 2 * k + 2 * LANE]
                    prod[rows, j + k : j + k + LANE] = (g * jax.nn.sigmoid(g) * u).astype(BF)
            return 0

        with jax.named_scope(f"products_{start}"):
            lax.fori_loop(0, tiles, products, 0)

    def gu_out(n):
        start, stop = pieces[n]
        return pltpu.make_async_copy(first[n], ogu[0].at[:, :, :, 2 * start : 2 * stop], out_sem.at[n])

    a_out = pltpu.make_async_copy(a, a_hbm, h_sem.at[tiles])
    a_out.start()
    outs = [gu_out(n) for n in range(len(pieces))] + [pltpu.make_async_copy(dd.at[0], od[0], out_sem.at[len(pieces)])]
    for layer in range(1, layers):
        for source, to in ((later.at[layer - 1], ogu[layer]), (dd.at[layer], od[layer])):
            half = source.shape[-1] // 2
            for owner in (core, 1 - core):
                cols = pl.ds(pl.multiple_of(owner * half, LANE), half)
                outs.append(pltpu.make_async_copy(source.at[:, :, :, cols], to.at[:, :, :, cols], out_sem.at[len(outs)]))
    down.finish(partner)
    for copy in outs[: len(pieces) + 1]:
        copy.start()
    r = dd.shape[3]
    for n in range(SIDE * SIDE):
        wide_d[r * n : r * (n + 1)] = dd[0, n // SIDE, n % SIDE].astype(F32)
    wd0[...] = wide_d[...].astype(BF)

    def tile_outs(t):
        rows = pl.ds(pl.multiple_of(t * FORWARD_TILE, FORWARD_TILE), FORWARD_TILE)
        return [pltpu.make_async_copy(xv.at[rows], h_hbm.at[rows], h_sem.at[t]), pltpu.make_async_copy(prod.at[rows], prod_hbm.at[rows], p_sem.at[t])]

    def close(t, _):
        for when, step in ((0, "D"), (tiles // 2, "E")):

            @pl.when(t == when)
            def _():
                go(step, *rest)
                if step == "E":
                    for copy in outs[len(pieces) + 1 :: 2]:
                        copy.start()

        rows = pl.ds(pl.multiple_of(t * FORWARD_TILE, FORWARD_TILE), FORWARD_TILE)
        xv[rows] = xv[rows] + dot(prod[rows], wd0[...]).astype(BF)
        for copy in tile_outs(t):
            copy.start()
        return 0

    with jax.named_scope("close"):
        lax.fori_loop(0, tiles, close, 0)
    for unit in rest:
        unit.finish(partner)
    for copy in outs[len(pieces) + 2 :: 2]:
        copy.start()
    for unit in units:
        unit.drain(partner)

    def closed(t, _):
        for copy in tile_outs(t):
            copy.wait()
        return 0

    with jax.named_scope("out_wait"):
        lax.fori_loop(0, tiles, closed, 0)
        for copy in outs + [a_out]:
            copy.wait()


def forward(x, wg, wu, wd):
    tokens, d = x.shape
    layers, rows, ff = wg.shape
    rows_d = wd.shape[1]
    pieces = pieces_of(ff)
    n = 17 * (len(pieces) + 2 * layers - 1)
    anywhere = pl.BlockSpec(memory_space=pl.ANY)
    h, a, prod, *full = pl.pallas_call(
        functools.partial(forward_kernel, layers),
        in_specs=[pl.BlockSpec(memory_space=pltpu.VMEM)] * 3 + [anywhere],
        out_specs=[anywhere] * (3 + 2 * layers),
        out_shape=[jax.ShapeDtypeStruct((tokens, d), BF)] * 2
        + [jax.ShapeDtypeStruct((tokens, ff), BF)]
        + [jax.ShapeDtypeStruct((SIDE, SIDE, rows, 2 * ff), BF)] * layers
        + [jax.ShapeDtypeStruct((SIDE, SIDE, rows_d, d), BF)] * layers,
        scratch_shapes=[pltpu.VMEM((SIDE, SIDE, rows, 2 * (stop - start)), BF) for start, stop in pieces]
        + [
            pltpu.VMEM((layers - 1, SIDE, SIDE, rows, 2 * ff), BF),
            pltpu.VMEM((layers, SIDE, SIDE, rows_d, d), BF),
            pltpu.VMEM((tokens, d), BF),
            pltpu.VMEM((tokens, d), BF),
            pltpu.VMEM((tokens, ff), BF),
            pltpu.VMEM((ff, d), F32),
            pltpu.VMEM((ff, d), BF),
            pltpu.SemaphoreType.DMA((n,)),
            pltpu.SemaphoreType.DMA((n,)),
            pltpu.SemaphoreType.DMA((len(pieces) + 4 * layers - 3,)),
            pltpu.SemaphoreType.DMA((tokens // FORWARD_TILE + 1,)),
            pltpu.SemaphoreType.DMA((tokens // FORWARD_TILE,)),
        ],
        compiler_params=pltpu.CompilerParams(collective_id=1, has_side_effects=True, vmem_limit_bytes=60 * 2**20),
    )(wg, wu, wd, x)
    return h, a, prod, [one.reshape(d, 2 * ff) for one in full[:layers]], [one.reshape(ff, d) for one in full[layers:]]


def hidden_back(both, by):
    g, u, b = both[:, :LANE], both[:, LANE:], by.astype(BF).astype(F32)
    s = jax.nn.sigmoid(g)
    silu = g * s
    return (b * u * (s + silu * (1 - s))).astype(BF), (b * silu).astype(BF), (silu * u).astype(BF)


def layer_kernel(h_ref, dy_ref, wgu_ref, wd_ref, dh_ref, dwgu_ref, dwd_ref, accgu, accd, dgu, prod):
    step, steps = pl.program_id(0), pl.num_programs(0)
    ff = wd_ref.shape[0]

    @pl.when(step == 0)
    def _():
        accgu[...] = jnp.zeros_like(accgu)
        accd[...] = jnp.zeros_like(accd)

    wide = h_ref[...].astype(F32)
    scale = inverse_rms(wide)
    a = (wide * scale).astype(BF)
    dy = dy_ref[...]
    for j in range(0, ff, 2 * LANE):
        c = min(2 * LANE, ff - j)
        both = dot(a, wgu_ref[:, 2 * j : 2 * (j + c)])
        by = dot(dy, wd_ref[j : j + c, :], 1, 1)
        for k in range(0, c, LANE):
            at = j + k
            dg, du, product = hidden_back(both[:, 2 * k : 2 * (k + LANE)], by[:, k : k + LANE])
            prod[:, at : at + LANE] = product
            dgu[:, 2 * at : 2 * at + LANE] = dg
            dgu[:, 2 * at + LANE : 2 * at + 2 * LANE] = du
    da = dot(dgu[...], wgu_ref[...], 1, 1)
    back = scale * (da - wide * (scale * scale * jnp.mean(da * wide, -1, keepdims=True)))
    dh_ref[...] = dy + back.astype(BF)
    accgu[...] += dot(a, dgu[...], 0, 0)
    accd[...] += dot(prod[...], dy, 0, 0)

    @pl.when(step == steps - 1)
    def _():
        r, q = dwgu_ref.shape[2], dwd_ref.shape[2]
        for d in range(SIDE * SIDE):
            dwgu_ref[d // SIDE, d % SIDE] = accgu[r * d : r * (d + 1)].astype(BF)
            dwd_ref[d // SIDE, d % SIDE] = accd[q * d : q * (d + 1)].astype(BF)


def layer_back(h, dy, wgu, wd):
    tokens, d = h.shape
    ff = wd.shape[0]
    n = SIDE * SIDE
    tile = pl.BlockSpec((TILE, d), lambda i: (i, 0))
    whole = lambda shape: pl.BlockSpec(shape, lambda i: (0,) * len(shape))
    gu, dd = (SIDE, SIDE, d // n, 2 * ff), (SIDE, SIDE, ff // n, d)
    return pl.pallas_call(
        layer_kernel,
        grid=(tokens // TILE,),
        in_specs=[tile, tile, whole(wgu.shape), whole(wd.shape)],
        out_specs=[tile, whole(gu), whole(dd)],
        out_shape=[jax.ShapeDtypeStruct((tokens, d), BF), jax.ShapeDtypeStruct(gu, BF), jax.ShapeDtypeStruct(dd, BF)],
        scratch_shapes=[
            pltpu.VMEM((d, 2 * ff), F32),
            pltpu.VMEM((ff, d), F32),
            pltpu.VMEM((TILE, 2 * ff), BF),
            pltpu.VMEM((TILE, ff), BF),
        ],
        compiler_params=pltpu.CompilerParams(vmem_limit_bytes=60 * 2**20),
    )(h, dy, wgu, wd)


class Scatter:
    def __init__(self, terms, bufs, send, recv, base):
        self.terms, self.send, self.recv, self.base = terms, send, recv, base
        self.a, self.b, self.sums, self.out, self.c, self.d = bufs
        self.half = terms.shape[-1] // 2
        r = terms.shape[2]
        if r % 32 == 0:
            self.parts = [(pl.ds(0, r // 2), slice(None)), (pl.ds(r // 2, r // 2), slice(None))]
        else:
            q = self.half // 2
            self.parts = [(slice(None), pl.ds(0, q)), (slice(None), pl.ds(q, q))]

    @staticmethod
    def scratch(rows, columns):
        half = columns // 2
        return [
            pltpu.VMEM((2, 2, SIDE // 2, rows, half), BF),
            pltpu.VMEM((2, 2, SIDE, rows, half), BF),
            pltpu.VMEM((2, SIDE, rows, half), F32),
            pltpu.VMEM((2, SIDE, rows, half), BF),
            pltpu.VMEM((2, rows, half), BF),
            pltpu.VMEM((2, 2, rows, half), BF),
        ]

    def index(self, which, first, second):
        cols = pl.ds(which * self.half, self.half)
        return (second, first, slice(None), cols) if which == 0 else (first, second, slice(None), cols)

    def copies(self, step):
        out = []
        for which, order in enumerate("yx"):
            i1, i2 = ring_places(order)
            for side in range(2):
                by = 1 - 2 * side
                if step == "A":
                    src = self.terms.at[self.index(which, shifted(i1, 2), pl.ds(side * (SIDE // 2), SIDE // 2))]
                    dst = self.a.at[which, side]
                elif step == "B":
                    src = self.terms.at[self.index(which, shifted(i1, by), slice(None))]
                    dst = self.b.at[which, side]
                elif step == "C":
                    rows, cols = self.parts[side]
                    src = self.out.at[which, shifted(i2, 2), rows, cols]
                    dst = self.c.at[which, rows, cols]
                else:
                    src = self.out.at[which, shifted(i2, by)]
                    dst = self.d.at[which, side]
                number = self.base + "ABCD".index(step) * 4 + which * 2 + side
                out.append(
                    pltpu.make_async_remote_copy(
                        src_ref=src,
                        dst_ref=dst,
                        send_sem=self.send.at[number],
                        recv_sem=self.recv.at[number],
                        device_id=along(order, by, step in "CD"),
                        device_id_type=MESH,
                    )
                )
        return out

    def advance(self, step):
        if step != "A":
            with jax.named_scope(f"wait_{step}{self.base // 16}"):
                for copy in self.copies("ABCD"["ABCDE".index(step) - 1]):
                    copy.wait_recv()
        for which, order in enumerate("yx"):
            i1, i2 = ring_places(order)
            if step == "B":
                for side in range(2):
                    for k in range(SIDE // 2):
                        at = self.index(which, shifted(i1, 1 - 2 * side), side * (SIDE // 2) + k)
                        self.terms[at] = (self.terms[at].astype(F32) + self.a[which, side, k].astype(F32)).astype(BF)
            elif step == "C":

                def own(k, _):
                    mine = self.terms[self.index(which, i1, k)].astype(F32)
                    self.sums[which, k] = mine + self.b[which, 0, k].astype(F32) + self.b[which, 1, k].astype(F32)
                    return 0

                lax.fori_loop(0, SIDE, own, 0)
                far = shifted(i2, 2)
                self.out[which, far] = self.sums[which, far].astype(BF)
            elif step == "D":
                for side in range(2):
                    near = shifted(i2, 1 - 2 * side)
                    for part in range(2):
                        at = self.parts[part]
                        value = self.sums[(which, near) + at]
                        if part == side:
                            value = value + self.c[(which,) + at].astype(F32)
                        self.out[(which, near) + at] = value.astype(BF)
        if step != "E":
            for copy in self.copies(step):
                copy.start()

    def result(self):
        halves = []
        for which, order in enumerate("yx"):
            _, i2 = ring_places(order)
            total = self.sums[which, i2] + self.d[which, 0].astype(F32) + self.d[which, 1].astype(F32)
            halves.append(total.astype(BF))
        return halves

    def drain(self):
        for step in "ABCD":
            for copy in self.copies(step):
                copy.wait_send()


class DirectScatter(Scatter):
    def __init__(self, terms, bufs, send, recv, base):
        self.terms, self.send, self.recv, self.base = terms, send, recv, base
        self.b, self.sums, self.out, self.d = bufs
        self.half = terms.shape[-1] // 2

    @staticmethod
    def scratch(rows, columns):
        half = columns // 2
        return [
            pltpu.VMEM((2, len(HOPS), SIDE, rows, half), BF),
            pltpu.VMEM((2, SIDE, rows, half), F32),
            pltpu.VMEM((2, SIDE, rows, half), BF),
            pltpu.VMEM((2, len(HOPS), rows, half), BF),
        ]

    def copies(self, step):
        out = []
        for which, order in enumerate("yx"):
            i1, i2 = ring_places(order)
            for k, by in enumerate(HOPS):
                if step == "A":
                    src, dst = self.terms.at[self.index(which, shifted(i1, by), slice(None))], self.b.at[which, k]
                else:
                    src, dst = self.out.at[which, shifted(i2, by)], self.d.at[which, k]
                number = self.base + (step == "C") * 6 + which * 3 + k
                out.append(
                    pltpu.make_async_remote_copy(
                        src_ref=src,
                        dst_ref=dst,
                        send_sem=self.send.at[number],
                        recv_sem=self.recv.at[number],
                        device_id=along(order, by, step == "C"),
                        device_id_type=MESH,
                    )
                )
        return out

    def advance(self, step):
        if step != "A":
            with jax.named_scope(f"wait_{step}{self.base // 16}"):
                for copy in self.copies("A" if step == "C" else "C"):
                    copy.wait_recv()
        if step == "C":
            for which, order in enumerate("yx"):
                i1, _ = ring_places(order)
                for k in range(SIDE):
                    total = self.terms[self.index(which, i1, k)].astype(F32)
                    for n in range(len(HOPS)):
                        total += self.b[which, n, k].astype(F32)
                    self.sums[which, k] = total
                    self.out[which, k] = total.astype(BF)
        if step != "E":
            for copy in self.copies(step):
                copy.start()

    def result(self):
        halves = []
        for which, order in enumerate("yx"):
            _, i2 = ring_places(order)
            total = self.sums[which, i2]
            for n in range(len(HOPS)):
                total += self.d[which, n].astype(F32)
            halves.append(total.astype(BF))
        return halves

    def drain(self):
        for step in "AC":
            for copy in self.copies(step):
                copy.wait_send()


def sum_everywhere(value, mine, theirs, send, recv, base, meanwhile):
    for which, order in enumerate("yx"):
        mine[which] = jnp.broadcast_to(value, mine.shape[1:])
        copies = [
            pltpu.make_async_remote_copy(
                src_ref=mine.at[which],
                dst_ref=theirs.at[which, by - 1],
                send_sem=send.at[base + which * 3 + by - 1],
                recv_sem=recv.at[base + which * 3 + by - 1],
                device_id=along(order, by),
                device_id_type=MESH,
            )
            for by in range(1, SIDE)
        ]
        with jax.named_scope(f"squares_{order}"):
            for copy in copies:
                copy.start()
            if which == 0:
                meanwhile()
            for copy in copies:
                copy.wait()
        value = value + theirs[which, 0][:1, :1] + theirs[which, 1][:1, :1] + theirs[which, 2][:1, :1]
    return value


def chunks_of(ff):
    cuts = [0, 4 * LANE, 8 * LANE, ff - LANE, ff]
    return list(zip(cuts[:-1], cuts[1:]))


def kinds_of(units):
    return [Scatter] * (units - 2) + [DirectScatter] * 2


def back_kernel(chunks, a_hbm, dh_hbm, wgu_hbm, wd_hbm, prod_hbm, gu_hbm, dd_hbm, rg_hbm, ru_hbm, rd_hbm, total, *refs):
    n_units = 3 + len(chunks)
    terms, refs = refs[:n_units], refs[n_units:]
    units = []
    for n, kind in enumerate(kinds_of(n_units)):
        count = len(kind.scratch(1, 2))
        units.append((kind, terms[n], refs[:count], 16 * n))
        refs = refs[count:]
    rg, ru, rd, a, dh, wgu, wd, pbuf, accd, accg, dgu, mine, theirs, send, recv, load, p_sem, out_sem = refs
    tokens, d = a.shape
    tiles = tokens // BACK_TILE
    units = [kind(term, bufs, send, recv, base) for kind, term, bufs, base in units]
    gu1, dd1, dd0, *parts = units
    pairs = [(gu_hbm, terms[0]), (dd_hbm, terms[1]), (dh_hbm, dh), (a_hbm, a), (wgu_hbm, wgu), (wd_hbm, wd)]
    loads = [pltpu.make_async_copy(source, to, load.at[n]) for n, (source, to) in enumerate(pairs)]
    rows_of = lambda t: pl.ds(pl.multiple_of(t * BACK_TILE, BACK_TILE), BACK_TILE)
    prod_load = lambda t: pltpu.make_async_copy(prod_hbm.at[rows_of(t)], pbuf.at[lax.rem(t, 2)], p_sem.at[lax.rem(t, 2)])
    for copy in loads[:3]:
        copy.start()
    prod_load(0).start()
    entry_barrier(others())
    for copy, unit in zip(loads[:2], units[:2], strict=True):
        copy.wait()
        unit.advance("A")
    loads[2].wait()
    accd[...] = jnp.zeros_like(accd)

    def down(t, _):
        @pl.when(t + 1 < tiles)
        def _():
            prod_load(t + 1).start()

        @pl.when(t == 0)
        def _():
            for copy in loads[3:]:
                copy.start()

        rows = rows_of(t)
        prod_load(t).wait()
        accd[...] += dot(pbuf[lax.rem(t, 2)], dh[rows], 0, 0)
        return 0

    with jax.named_scope("down"):
        lax.fori_loop(0, tiles, down, 0)
    q = terms[2].shape[2]
    for n in range(SIDE * SIDE):
        terms[2][n // SIDE, n % SIDE] = accd[q * n : q * (n + 1)].astype(BF)
    gu1.advance("B")
    for copy in loads[3:]:
        copy.wait()
    one, two, three, four = parts
    slots = [
        {4: [(dd1, "B"), (dd0, "A")]},
        {0: [(gu1, "C"), (one, "A")], 2: [(dd1, "C"), (dd0, "B")], 4: [(gu1, "D"), (one, "B")], 6: [(dd1, "D"), (dd0, "C")]},
        {0: [(two, "A")], 2: [(one, "C"), (dd0, "D")], 4: [(two, "B")], 6: [(one, "D")]},
        {0: [(three, "A")], 4: [(two, "C")]},
    ]
    for (start, stop), term, slot in zip(chunks, terms[3:], slots, strict=True):
        width = 2 * (stop - start)
        tile = BACK_TILE if stop < chunks[-1][1] else 2 * BACK_TILE
        tiles = tokens // tile
        accg[:, :width] = jnp.zeros((d, width), F32)

        def chunk(t, _):
            for when, actions in slot.items():

                @pl.when(t == when * tiles // 8)
                def _():
                    for unit, step in actions:
                        unit.advance(step)

            rows = pl.ds(pl.multiple_of(t * tile, tile), tile)
            at, by = a[rows], dh[rows]
            to_rows = pl.ds(0, tile)
            for j in range(start, stop, 2 * LANE):
                c = min(2 * LANE, stop - j)
                both = dot(at, wgu[:, 2 * j : 2 * (j + c)])
                back = dot(by, wd[j : j + c, :], 1, 1)
                for k in range(0, c, LANE):
                    dg, du, _ = hidden_back(both[:, 2 * k : 2 * (k + LANE)], back[:, k : k + LANE])
                    to = 2 * (j - start + k)
                    dgu[to_rows, to : to + LANE] = dg
                    dgu[to_rows, to + LANE : to + 2 * LANE] = du
            accg[:, :width] += dot(at, dgu[to_rows, :width], 0, 0)
            return 0

        with jax.named_scope(f"chunk_{start}"):
            lax.fori_loop(0, tiles, chunk, 0)
        r = term.shape[2]
        for n in range(SIDE * SIDE):
            term[n // SIDE, n % SIDE] = accg[r * n : r * (n + 1), :width].astype(BF)
    four.advance("A")
    squares = jnp.zeros((1, 1), F32)

    def taken(unit, layer, start):
        unit.advance("E")
        found = jnp.zeros((1, 1), F32)
        for which, half in enumerate(unit.result()):
            wide = half.astype(F32)
            found += jnp.sum(wide * wide, keepdims=True)
            width = half.shape[1]
            if start is None:
                rd[layer, :, which * width : (which + 1) * width] = half
            else:
                for k in range(0, width, LANE):
                    block = (2 * start + which * width + k) // LANE
                    out = (rg, ru)[block % 2]
                    out[layer, :, block // 2 * LANE : (block // 2 + 1) * LANE] = half[:, k : k + LANE]
        return found

    starts = [start for start, _ in chunks]
    three.advance("C")
    two.advance("D")
    squares += taken(gu1, 1, 0) + taken(dd1, 1, None)
    four.advance("C")
    squares += taken(dd0, 0, None) + taken(one, 0, starts[0])
    squares += taken(two, 0, starts[1]) + taken(three, 0, starts[2])
    squares += taken(four, 0, starts[3])
    outs = [pltpu.make_async_copy(source, to, out_sem.at[n]) for n, (source, to) in enumerate(((rg, rg_hbm), (ru, ru_hbm), (rd, rd_hbm)))]

    def meanwhile():
        for copy in outs:
            copy.start()
        for unit in units:
            unit.drain()

    total[...] = jnp.broadcast_to(sum_everywhere(squares, mine, theirs, send, recv, 16 * n_units, meanwhile), total.shape)
    for copy in outs:
        copy.wait()


def back_and_reduced(a, dh, wgu, wd, prod, gu, dd):
    tokens, d = a.shape
    ff = wd.shape[0]
    rows, rows_d = gu.shape[2], dd.shape[2]
    chunks = chunks_of(ff)
    shapes = [gu.shape, dd.shape, dd.shape] + [gu.shape[:3] + (2 * (stop - start),) for start, stop in chunks]
    widest = 2 * max(stop - start for start, stop in chunks)
    scratch = [pltpu.VMEM(shape, BF) for shape in shapes]
    for shape, kind in zip(shapes, kinds_of(len(shapes)), strict=True):
        scratch += kind.scratch(shape[2], shape[3])
    n = 16 * len(shapes) + 6
    return pl.pallas_call(
        functools.partial(back_kernel, chunks),
        in_specs=[pl.BlockSpec(memory_space=pl.ANY)] * 7,
        out_specs=[pl.BlockSpec(memory_space=pl.ANY)] * 3 + [pl.BlockSpec(memory_space=pltpu.VMEM)],
        out_shape=[
            jax.ShapeDtypeStruct((2, rows, ff), BF),
            jax.ShapeDtypeStruct((2, rows, ff), BF),
            jax.ShapeDtypeStruct((2, rows_d, d), BF),
            jax.ShapeDtypeStruct((8, LANE), F32),
        ],
        scratch_shapes=scratch
        + [
            pltpu.VMEM((2, rows, ff), BF),
            pltpu.VMEM((2, rows, ff), BF),
            pltpu.VMEM((2, rows_d, d), BF),
            pltpu.VMEM((tokens, d), BF),
            pltpu.VMEM((tokens, d), BF),
            pltpu.VMEM((d, 2 * ff), BF),
            pltpu.VMEM((ff, d), BF),
            pltpu.VMEM((2, BACK_TILE, ff), BF),
            pltpu.VMEM((ff, d), F32),
            pltpu.VMEM((d, widest), F32),
            pltpu.VMEM((2 * BACK_TILE, widest), BF),
            pltpu.VMEM((2, 8, LANE), F32),
            pltpu.VMEM((2, SIDE - 1, 8, LANE), F32),
            pltpu.SemaphoreType.DMA((n,)),
            pltpu.SemaphoreType.DMA((n,)),
            pltpu.SemaphoreType.DMA((6,)),
            pltpu.SemaphoreType.DMA((2,)),
            pltpu.SemaphoreType.DMA((3,)),
        ],
        compiler_params=pltpu.CompilerParams(collective_id=2, has_side_effects=True, vmem_limit_bytes=62 * 2**20),
    )(a, dh, wgu, wd, prod, gu, dd)


def adamw(w, m, v, g):
    m = 0.9 * m + 0.1 * g
    v = 0.95 * v + 0.05 * g * g
    step = m * lax.rsqrt(v + 1e-8) + 0.1 * w
    return (w - 0.02 * step).astype(jnp.bfloat16), m, v


def update_kernel(count, total_ref, *refs):
    inputs, outputs = refs[:12], refs[12:]
    factor = jnp.minimum(1.0, 0.5 * lax.rsqrt(total_ref[:1, :1] / count + 1e-30))
    for i in range(3):
        w, m, v, g = inputs[i::3]
        for layer in range(w.shape[0]):
            new = adamw(w[layer].astype(F32), m[layer], v[layer], g[layer].astype(F32) * factor)
            for to, value in zip(outputs[i::3], new, strict=True):
                to[layer] = value


def updated(count, total, weights, m, v, gradients):
    inputs = [*weights, *m, *v, *gradients]
    return pl.pallas_call(
        functools.partial(update_kernel, count),
        in_specs=[pl.BlockSpec(memory_space=pltpu.VMEM)] * 13,
        out_specs=[pl.BlockSpec(memory_space=pltpu.VMEM)] * 9,
        out_shape=[jax.ShapeDtypeStruct(one.shape, one.dtype) for one in inputs[:9]],
        compiler_params=pltpu.CompilerParams(vmem_limit_bytes=62 * 2**20),
    )(total, *inputs)


def solution(mesh):
    group = mesh.shape["dp"]

    def step(x, dy, *arrays):
        weights, m, v = (arrays[i : i + 3] for i in (0, 3, 6))
        h0, by1 = x[0], dy[0]
        h1, a0, prod, wgu, wd = forward(h0, *weights)
        by0, gu1, dd1 = layer_back(h1, by1, wgu[1], wd[1])
        *gradients, total = back_and_reduced(a0, by0, wgu[0], wd[0], prod, gu1, dd1)
        count = group * sum(g.size for g in gradients)
        return tuple(updated(count, total, weights, m, v, gradients))

    states, cut = P(("rep", "dp"), None, None), P(None, "dp", None)
    return jax.shard_map(
        step,
        mesh=mesh,
        in_specs=(states, states) + (cut,) * 9,
        out_specs=(P("rep", "dp", None),) * 9,
        check_vma=False,
    )
```
